256 devices in a mesh: row: 8 (over z_lo, x), col: 32 (over z_hi, y, core).
Axes of the slice: x: 4, y: 4, z: 8 (z_hi: 4, z_lo: 2; z = z_hi * 2 + z_lo), core: 2. Of those that a mesh axis runs over, the one named last changes fastest.
Arguments:
- upper_a: float32 [4, 8, 256, 32, 256], P(None, 'row', None, 'col'), may hold values from -0.375 to 0.375
- upper_b: float32 [4, 8, 256, 32, 256], P(None, 'row', None, 'col'), may hold values from -0.375 to 0.375
- right_side: float32 [4, 8, 256, 32, 256], P(None, 'row', None, 'col'), may hold values from -6 to 6
- vectors_a: float32 [4, 8, 256, 256], P(None, 'row'), may hold values from -0.375 to 0.375
- inverse_a: float32 [4, 8, 256, 256], P(None, 'row'), may hold values from -0.375 to 0.375
- values_a: float32 [4, 8, 256], P(None, 'row'), may hold values from 0.5 to 2
- vectors_b: float32 [32, 256, 256], P('col'), may hold values from -0.375 to 0.375
- inverse_b: float32 [32, 256, 256], P('col'), may hold values from -0.375 to 0.375
- values_b: float32 [32, 256], P('col'), may hold values from 0.5 to 2
Outputs:
- solved: float32 [4, 8, 256, 32, 256], P(None, 'row', None, 'col')
The draws below stay inside these ranges and needn't reach their ends.
All inputs are finite; a program needn't handle non-finite values.
Results may differ from the reference program's by a relative error of at most 0.0001.
Values sent between devices are 32-bit elements; how exact they have to be, the bound alone decides.
A program may use at most 64 MiB of HBM per device.

```python
import math
import jax
import jax.numpy as jnp
from jax import lax

BLOCK = 256
FRONTS = 4
BLOCKS = 32
ROW_BLOCKS = 4
N_ROW = 8
N_COL = 32


def block_scale(own_key, shape, cuts, least, top_value):
    gain, own = 1.0, jax.random.fold_in(own_key, 6)
    for position, blocks in cuts:
        steps = jnp.exp(jax.random.uniform(jax.random.fold_in(own, position), (blocks,), jnp.float32, least / len(cuts), top_value / len(cuts)))
        gain = gain * jnp.repeat(steps, shape[position] // blocks).reshape([-1 if axis == position else 1 for axis in range(len(shape))])
    return gain


def normal_values(stream_key, shape, deviation, limit, cuts=(), kind=jnp.bfloat16):
    drawn = jax.random.normal(stream_key, shape, jnp.float32) * deviation
    if len(cuts) > 0:
        drawn = block_scale(stream_key, shape, cuts, -0.22, 0.18) * drawn
    return jnp.clip(drawn, min=-limit, max=limit).astype(kind)


def setup_inputs(seed: int = 0) -> dict:
    key_of = jax.random.split(jax.random.key(seed), 10)
    return {
        "upper_a": normal_values(key_of[0], (ROW_BLOCKS, N_ROW, BLOCK, N_COL, BLOCK), BLOCK ** -0.5, 0.375, ((1, 8), (3, 32)), jnp.float32),
        "upper_b": normal_values(key_of[1], (ROW_BLOCKS, N_ROW, BLOCK, N_COL, BLOCK), BLOCK ** -0.5, 0.375, ((1, 8), (3, 32)), jnp.float32),
        "right_side": normal_values(key_of[2], (ROW_BLOCKS, N_ROW, BLOCK, N_COL, BLOCK), 1.0, 6.0, ((1, 8), (3, 32)), jnp.float32),
        "vectors_a": normal_values(key_of[3], (ROW_BLOCKS, N_ROW, BLOCK, BLOCK), BLOCK ** -0.5, 0.375, ((1, 8),), jnp.float32),
        "inverse_a": normal_values(key_of[4], (ROW_BLOCKS, N_ROW, BLOCK, BLOCK), BLOCK ** -0.5, 0.375, ((1, 8),), jnp.float32),
        "values_a": jnp.clip(jnp.exp(math.log(2.0) - 1.3862944 * jax.random.uniform(key_of[5], (ROW_BLOCKS, N_ROW, BLOCK), jnp.float32) ** block_scale(key_of[5], (ROW_BLOCKS, N_ROW, BLOCK), ((1, 8),), -0.2, 0.2)), 0.5, 2.0),
        "vectors_b": normal_values(key_of[6], (BLOCKS, BLOCK, BLOCK), BLOCK ** -0.5, 0.375, ((0, 32),), jnp.float32),
        "inverse_b": normal_values(key_of[7], (BLOCKS, BLOCK, BLOCK), BLOCK ** -0.5, 0.375, ((0, 32),), jnp.float32),
        "values_b": jnp.clip(jnp.exp(math.log(2.0) - 1.3862944 * jax.random.uniform(key_of[8], (BLOCKS, BLOCK), jnp.float32) ** block_scale(key_of[8], (BLOCKS, BLOCK), ((0, 32),), -0.2, 0.2)), 0.5, 2.0),
    }


EXACT = lax.Precision.HIGHEST


def matmul(former, latter):
    return jnp.dot(former, latter, precision=EXACT, preferred_element_type=jnp.float32)


def diagonal_solve(residual, vectors_a, inverse_a, values_a, vectors_b, inverse_b, values_b):
    rotated = matmul(matmul(inverse_a, residual), vectors_b)
    scaled = rotated / (values_a[:, None] + values_b[None, :])
    return matmul(matmul(vectors_a, scaled), inverse_b)


def reference(upper_a, upper_b, right_side, vectors_a, inverse_a, values_a, vectors_b, inverse_b, values_b):
    block_grid = (BLOCKS, BLOCK, BLOCKS, BLOCK)
    matrix_a = upper_a.reshape(block_grid)
    matrix_b = upper_b.reshape(block_grid)
    work = right_side.reshape(block_grid)
    left_vectors = vectors_a.reshape(BLOCKS, BLOCK, BLOCK)
    left_inverse = inverse_a.reshape(BLOCKS, BLOCK, BLOCK)
    left_values = values_a.reshape(BLOCKS, BLOCK)
    block_ids = jnp.arange(BLOCKS, dtype=jnp.int32)
    diagonal_gap = block_ids[None, :] - block_ids[:, None]
    for front_step in range(FRONTS):
        offset = front_step - 1
        partner = block_ids + offset
        inside = (partner >= 0) & (partner < BLOCKS)
        partner_clip = jnp.clip(partner, 0, BLOCKS - 1).astype(jnp.int32)
        residual = work[block_ids, :, partner_clip, :]
        solved = jax.vmap(diagonal_solve)(residual, left_vectors, left_inverse, left_values,
                                          vectors_b[partner_clip], inverse_b[partner_clip], values_b[partner_clip])
        solved = jnp.where(inside[:, None, None], solved, jnp.zeros_like(solved))
        on_front = diagonal_gap == offset
        placed = solved[:, :, None, :] * on_front[:, None, :, None].astype(jnp.float32)
        work = jnp.where(on_front[:, None, :, None], placed, work)
        source = block_ids - offset
        source_valid = (source >= 0) & (source < BLOCKS)
        source_clip = jnp.clip(source, 0, BLOCKS - 1).astype(jnp.int32)
        column_solved = jnp.where(source_valid[:, None, None], solved[source_clip], jnp.zeros_like(solved))
        upper_panel = matrix_a[:, :, source_clip, :]
        upper_term = jnp.einsum("ixjy,jyz->ixjz", upper_panel, column_solved, precision=EXACT)
        lower_rows = matrix_b[partner_clip]
        lower_term = jnp.einsum("ixy,iyjz->ixjz", solved, lower_rows, precision=EXACT)
        pending = diagonal_gap > offset
        work = jnp.where(pending[:, None, :, None], work - (upper_term + lower_term), work)
    return work.reshape(right_side.shape)
```

```python
import functools

import jax
import jax.numpy as jnp
from jax import lax
from jax.experimental import pallas as pl
from jax.experimental.pallas import tpu as pltpu
from jax.sharding import Mesh
from jax.sharding import PartitionSpec as P

FRONTS = 4
N_SLOT = 4
BLOCK = 256
HALF = 128
N_COL = 32
MESH = pl.DeviceIdType.MESH
ROW = ("zl", "x")
COL = ("zh", "y", "k")


def parts(value):
    high = value.astype(jnp.bfloat16)
    low = (value - high.astype(jnp.float32)).astype(jnp.bfloat16)
    return high, low


def matmul(former, latter):
    former_high, former_low = parts(former)
    latter_high, latter_low = parts(latter)
    left = jnp.concatenate([former_high, former_low, former_high], axis=1)
    right = jnp.concatenate([latter_high, latter_high, latter_low], axis=0)
    return jnp.dot(left, right, preferred_element_type=jnp.float32)


def kernel(
    a_hbm, b_hbm, w_hbm, va_hbm, ia_hbm, la_ref, vb_hbm, ib_hbm, lb_ref, out_hbm,
    a_all, b_all, work, x_col, x_row, va, ia, vb, ib, denominator,
    a_send, a_recv, b_send, b_recv, row_send, row_far, row_recv, col_send, col_recv, local, out_sem,
):
    zl, x = lax.axis_index("zl"), lax.axis_index("x")
    zh, y, k = lax.axis_index("zh"), lax.axis_index("y"), lax.axis_index("k")
    r = zl * 4 + x
    c = zh * 8 + y * 2 + k
    rem, div = lax.rem, lax.div

    def place(zl=zl, x=x, zh=zh, y=y, k=k):
        return {"zl": zl, "x": x, "zh": zh, "y": y, "k": k}

    def at_column(j):
        return place(zh=div(j, 8), y=div(rem(j, 8), 2), k=rem(j, 2))

    def at_row(i):
        return place(zl=div(i, 4), x=rem(i, 4))

    def remote(src, dst, send_sem, recv_sem, where):
        return pltpu.make_async_remote_copy(
            src_ref=src, dst_ref=dst, send_sem=send_sem, recv_sem=recv_sem,
            device_id=where, device_id_type=MESH,
        )

    own_front = rem(c - r + 33, 8)
    own_slot = div(c - r - own_front + 1 + 64, 8) - 8
    owner = (own_front < FRONTS) & (own_slot >= 0) & (own_slot < N_SLOT)
    slot = jnp.clip(own_slot, 0, N_SLOT - 1)

    loads = [
        pltpu.make_async_copy(w_hbm, work, local.at[0]),
        pltpu.make_async_copy(a_hbm, a_all.at[1], local.at[1]),
        pltpu.make_async_copy(b_hbm, b_all.at[1], local.at[2]),
    ]
    factor_loads = [
        pltpu.make_async_copy(ia_hbm.at[slot], ia, local.at[3]),
        pltpu.make_async_copy(vb_hbm, vb, local.at[4]),
        pltpu.make_async_copy(va_hbm.at[slot], va, local.at[5]),
        pltpu.make_async_copy(ib_hbm, ib, local.at[6]),
    ]
    loads[0].start()

    @pl.when(owner)
    def _():
        for load in factor_loads:
            load.start()

    loads[1].start()
    loads[2].start()

    barrier = pltpu.get_barrier_semaphore()
    friends = [at_column(rem(c + by, N_COL)) for by in (1, 31, 2, 30)]
    friends += [at_row(rem(r + by, 8)) for by in (1, 7)]
    friends += [place(zl=1 - zl), place(x=rem(x + 1, 4)), place(x=rem(x + 3, 4))]
    friends += [place(k=1 - k), place(y=rem(y + 1, 4)), place(y=rem(y + 3, 4))]
    friends += [place(zh=rem(zh + by, 4)) for by in (1, 2, 3)]
    for friend in friends:
        pl.semaphore_signal(barrier, inc=1, device_id=friend, device_id_type=MESH)

    @pl.when(owner)
    def _():
        left = jnp.concatenate(
            [la_ref[pl.ds(2 * slot, 1), :], la_ref[pl.ds(2 * slot + 1, 1), :]], axis=1
        )
        right = jnp.concatenate([lb_ref[pl.ds(0, 1), :], lb_ref[pl.ds(1, 1), :]], axis=1)
        denominator[...] = jnp.broadcast_to(left, (BLOCK, BLOCK)).T + right
        for load in factor_loads:
            load.wait()

    pl.semaphore_wait(barrier, len(friends))
    for load in loads:
        load.wait()

    def block_of(ref, *index):
        return jnp.concatenate(
            [ref[(*index, pl.ds(0, BLOCK, 2), slice(None))], ref[(*index, pl.ds(1, BLOCK, 2), slice(None))]],
            axis=1,
        )

    def put_work(q, value):
        work[q, pl.ds(0, BLOCK, 2), :] = value[:, :HALF]
        work[q, pl.ds(1, BLOCK, 2), :] = value[:, HALF:]

    def shift_copies(q):
        above = 8 * q + r < c
        up_slot = jnp.minimum(q + div(r, 7), N_SLOT - 1)
        first_row = jnp.where(r == 0, 1, 0)
        down_slot = jnp.maximum(q - first_row, 0)
        yield above, remote(
            a_hbm.at[q], a_all.at[0, q], a_send.at[0, q], a_recv.at[0, q], at_column(jnp.maximum(c - 1, 0))
        )
        yield above, remote(
            b_hbm.at[q], b_all.at[0, up_slot], b_send.at[0, q], b_recv.at[0, up_slot], at_row(rem(r + 1, 8))
        )
        yield above & (c + 1 < N_COL), remote(
            a_hbm.at[q], a_all.at[2, q], a_send.at[2, q], a_recv.at[2, q], at_column(jnp.minimum(c + 1, N_COL - 1))
        )
        yield above & (8 * q + r > 0), remote(
            b_hbm.at[q], b_all.at[2, down_slot], b_send.at[2, q], b_recv.at[2, down_slot], at_row(rem(r + 7, 8))
        )
        yield above & (c + 2 < N_COL) & (k == 0), remote(
            a_hbm.at[q], a_all.at[3, q], a_send.at[3, q], a_recv.at[3, q], at_column(jnp.minimum(c + 2, N_COL - 1))
        )

    def passed_copies(q):
        above = 8 * q + r + 1 < c
        first_row = jnp.where(r == 0, 1, 0)
        down_slot = jnp.maximum(q - first_row, 0)
        here = 8 * q + r < c - 1
        yield here, here & (k == 0), remote(
            a_all.at[2, q], a_all.at[3, q], a_send.at[1, q], a_recv.at[3, q], place(k=1 - k)
        ), remote(a_all.at[2, q], a_all.at[2, q], a_send.at[2, q], a_recv.at[2, q], place(k=1 - k))
        yield above, above & (8 * q + r > 0), remote(
            b_all.at[2, q], b_all.at[3, down_slot], b_send.at[3, q], b_recv.at[3, down_slot], at_row(rem(r + 7, 8))
        ), remote(b_all.at[2, q], b_all.at[2, q], b_send.at[2, q], b_recv.at[2, q], at_row(rem(r + 7, 8)))

    def column_role(f):
        i0 = c - f + 1
        exists = (i0 >= 0) & (i0 < N_COL)
        r0 = rem(i0 + 8, 8)
        dx = rem(x - rem(r0, 4) + 4, 4)
        same = zl == div(r0, 4)
        return exists, dx, same

    def column_copies(f, t):
        exists, dx, same = column_role(f)
        half = x_col.at[f, pl.ds(t * HALF, HALF), :]

        def to(n, where):
            return remote(half, half, col_send.at[f, t, n], col_recv.at[f, t], where)

        outer = 1 if t == 0 else 3
        yield exists & (dx == 0) & same, to(0, place(zl=1 - zl))
        if t == 0:
            yield exists & (dx <= 1), to(1, place(x=rem(x + 1, 4)))
            yield exists & (dx == 0), to(2, place(x=rem(x + 3, 4)))
        else:
            yield exists & (dx == 0), to(1, place(x=rem(x + 1, 4)))
            yield exists & ((dx == 0) | (dx == outer)), to(2, place(x=rem(x + 3, 4)))

    def column_arrival(f, t):
        exists, dx, same = column_role(f)
        half = x_col.at[f, pl.ds(t * HALF, HALF), :]
        source = (dx == 0) & same
        return exists & jnp.logical_not(source), remote(
            half, half, col_send.at[f, t, 0], col_recv.at[f, t], place(zl=1 - zl)
        )

    def row_role(f, q):
        total = r + f + 7
        place_in = rem(total, 8)
        plane = q + div(total, 8) - 1
        dy = rem(y - div(place_in, 2) + 4, 4)
        same = k == rem(place_in, 2)
        return plane, (plane >= 0) & (plane <= zh), dy, same

    def row_copies(f, q, t):
        plane, present, dy, same = row_role(f, q)
        half = x_row.at[f, q, pl.ds(t * HALF, HALF), :]

        def to(sem, where):
            return remote(half, half, sem, row_recv.at[f, q, t], where)

        carrier = present & same
        yield carrier, to(row_send.at[f, q, t, 0], place(k=1 - k))
        first, last = (dy <= 1, dy == 0) if t == 0 else (dy == 0, (dy == 0) | (dy == 3))
        yield carrier & first, to(row_send.at[f, q, t, 1], place(y=rem(y + 1, 4)))
        yield carrier & last, to(row_send.at[f, q, t, 2], place(y=rem(y + 3, 4)))

    def far_copies(f, q, t):
        half = x_row.at[f, q, pl.ds(t * HALF, HALF), :]
        for by in (1, 2, 3):
            yield zh + by < 4, remote(
                half, half, row_far.at[t, by - 1], row_recv.at[f, q, t], place(zh=jnp.minimum(zh + by, 3))
            )

    def row_arrival(f, q, t):
        plane, present, dy, same = row_role(f, q)
        half = x_row.at[f, q, pl.ds(t * HALF, HALF), :]
        source = (plane == zh) & (dy == 0) & same
        return present & jnp.logical_not(source), remote(
            half, half, row_send.at[f, q, t, 0], row_recv.at[f, q, t], place(k=1 - k)
        )

    def start(condition, copy):
        @pl.when(condition)
        def _():
            copy.start()

    def drain(condition, copy):
        @pl.when(condition)
        def _():
            copy.wait_send()

    def land(condition, copy):
        @pl.when(condition)
        def _():
            copy.wait_recv()

    def update(f, q):
        upper = c - f + 1 < N_COL
        lower = 8 * q + r + f - 1 >= 0
        early = (f == 0) | (f == 3)
        land(upper & early, remote(a_all.at[f, q], a_all.at[f, q], a_send.at[f, q], a_recv.at[f, q], place(k=1 - k)))
        land(lower & early, remote(b_all.at[f, q], b_all.at[f, q], b_send.at[f, q], b_recv.at[f, q], place(k=1 - k)))

        @pl.when(upper)
        def _():
            put_work(q, block_of(work, q) - matmul(block_of(a_all, f, q), x_col[f]))

        @pl.when(lower)
        def _():
            put_work(q, block_of(work, q) - matmul(x_row[f, q], block_of(b_all, f, q)))

    def bulk(f):
        def one(q, carry):
            done_before = owner & (q == own_slot)

            @pl.when((c - 8 * q - r >= f) & jnp.logical_not(done_before))
            def _():
                update(f, q)

            return carry

        lax.fori_loop(0, N_SLOT, one, 0)

    def front(f, carry):
        @pl.when(owner & (own_front == f))
        def _():
            rotated = matmul(matmul(ia[...], block_of(work, slot)), vb[...])
            solved = matmul(matmul(va[...], rotated / denominator[...]), ib[...])
            x_col[f] = solved
            x_row[f, slot] = solved
            put_work(slot, solved)
            for t in (0, 1):
                for condition, copy in column_copies(f, t):
                    start(condition, copy)
                for condition, copy in row_copies(f, slot, t):
                    start(condition, copy)
            for t in (0, 1):
                for condition, copy in far_copies(f, slot, t):
                    start(condition, copy)

        @pl.when(f == 0)
        def _():
            def one(step, carry):
                for condition, copy in shift_copies(N_SLOT - 1 - step):
                    start(condition, copy)
                return carry

            lax.fori_loop(0, N_SLOT, one, 0)

        @pl.when(f > 0)
        def _():
            bulk(f - 1)

        for t in (0, 1):
            arriving, arrival = column_arrival(f, t)

            @pl.when(arriving)
            def _():
                arrival.wait_recv()
                for condition, copy in column_copies(f, t):
                    start(condition, copy)

        def hand_on(step, carry):
            q = N_SLOT - 1 - step
            for t in (0, 1):
                arriving, arrival = row_arrival(f, q, t)

                @pl.when(arriving)
                def _():
                    arrival.wait_recv()
                    for condition, copy in row_copies(f, q, t):
                        start(condition, copy)

            return carry

        lax.fori_loop(0, N_SLOT, hand_on, 0)

        @pl.when(owner & (f < own_front))
        def _():
            update(f, slot)

        @pl.when(f == 1)
        def _():
            def one(step, carry):
                for arrived, forwarded, copy, arrival in passed_copies(N_SLOT - 1 - step):
                    land(arrived, arrival)
                    start(forwarded, copy)
                return carry

            lax.fori_loop(0, N_SLOT, one, 0)

        return carry

    lax.fori_loop(0, FRONTS, front, 0)
    bulk(FRONTS - 1)

    result = pltpu.make_async_copy(work, out_hbm, out_sem)
    result.start()

    def finish(q, carry):
        for condition, copy in shift_copies(q):
            drain(condition, copy)
        for _, forwarded, copy, _ in passed_copies(q):
            drain(forwarded, copy)
        return carry

    lax.fori_loop(0, N_SLOT, finish, 0)

    def finish_front(f, carry):
        for t in (0, 1):
            for condition, copy in column_copies(f, t):
                drain(condition, copy)

        def one(q, carry):
            for t in (0, 1):
                for condition, copy in row_copies(f, q, t):
                    drain(condition, copy)
            return carry

        return lax.fori_loop(0, N_SLOT, one, carry)

    lax.fori_loop(0, FRONTS, finish_front, 0)

    @pl.when(owner)
    def _():
        for t in (0, 1):
            for condition, copy in far_copies(own_front, slot, t):
                drain(condition, copy)

    result.wait()


def body(
    upper_a, upper_b, right_side, vectors_a, inverse_a, values_a, vectors_b, inverse_b, values_b
):
    tall = (N_SLOT, 2 * BLOCK, HALF)
    square = (N_SLOT, BLOCK, BLOCK)
    anywhere = pl.BlockSpec(memory_space=pl.ANY)
    inside = pl.BlockSpec(memory_space=pltpu.VMEM)
    dma = pltpu.SemaphoreType.DMA
    solved = pl.pallas_call(
        kernel,
        out_shape=jax.ShapeDtypeStruct(tall, jnp.float32),
        in_specs=[anywhere] * 5 + [inside] + [anywhere] * 2 + [inside],
        out_specs=anywhere,
        scratch_shapes=[
            pltpu.VMEM((FRONTS, *tall), jnp.float32),
            pltpu.VMEM((FRONTS, *tall), jnp.float32),
            pltpu.VMEM(tall, jnp.float32),
            pltpu.VMEM(square, jnp.float32),
            pltpu.VMEM((FRONTS, *square), jnp.float32),
            *[pltpu.VMEM((BLOCK, BLOCK), jnp.float32)] * 5,
            dma((4, N_SLOT)),
            dma((4, N_SLOT)),
            dma((4, N_SLOT)),
            dma((4, N_SLOT)),
            dma((FRONTS, N_SLOT, 2, 3)),
            dma((2, 3)),
            dma((FRONTS, N_SLOT, 2)),
            dma((FRONTS, 2, 3)),
            dma((FRONTS, 2)),
            dma((7,)),
            dma,
        ],
        compiler_params=pltpu.CompilerParams(
            collective_id=0, has_side_effects=True, vmem_limit_bytes=48 * 1024 * 1024
        ),
    )(
        upper_a.reshape(tall), upper_b.reshape(tall), right_side.reshape(tall),
        vectors_a.reshape(square), inverse_a.reshape(square), values_a.reshape(2 * N_SLOT, HALF),
        vectors_b.reshape(BLOCK, BLOCK), inverse_b.reshape(BLOCK, BLOCK), values_b.reshape(2, HALF),
    )
    return solved.reshape(right_side.shape)


def solution(mesh):
    finer = Mesh(mesh.devices.reshape(2, 4, 4, 4, 2), ROW + COL)
    whole = P(None, ROW, None, COL, None)
    placed = (
        whole, whole, whole,
        P(None, ROW, None, None), P(None, ROW, None, None), P(None, ROW, None),
        P(COL, None, None), P(COL, None, None), P(COL, None),
    )
    return jax.shard_map(body, mesh=finer, in_specs=placed, out_specs=whole, check_vma=False)
```

```python
import functools

import jax
import jax.numpy as jnp
from jax import lax
from jax.experimental import pallas as pl
from jax.experimental.pallas import tpu as pltpu
from jax.sharding import Mesh
from jax.sharding import PartitionSpec as P

FRONTS = 4
N_SLOT = 4
BLOCK = 256
HALF = 128
N_COL = 32
MESH = pl.DeviceIdType.MESH
ROW = ("zl", "x")
COL = ("zh", "y", "k")


def parts(value):
    high = value.astype(jnp.bfloat16)
    low = (value - high.astype(jnp.float32)).astype(jnp.bfloat16)
    return high, low


def matmul(former, latter):
    former_high, former_low = parts(former)
    latter_high, latter_low = parts(latter)
    left = jnp.concatenate([former_high, former_low, former_high], axis=1)
    right = jnp.concatenate([latter_high, latter_high, latter_low], axis=0)
    return jnp.dot(left, right, preferred_element_type=jnp.float32)


def kernel(
    a_hbm, b_hbm, w_hbm, va_hbm, ia_hbm, la_ref, vb_hbm, ib_hbm, lb_ref, out_hbm,
    a_all, b_all, work, x_col, x_row, chain_col, chain_row, va, ia, vb, ib, denominator,
    a_send, a_recv, b_send, b_recv, row_send, row_far, row_recv, col_send, col_recv, chain_send, chain_recv, local, out_sem,
):
    zl, x = lax.axis_index("zl"), lax.axis_index("x")
    zh, y, k = lax.axis_index("zh"), lax.axis_index("y"), lax.axis_index("k")
    r = zl * 4 + x
    c = zh * 8 + y * 2 + k
    rem, div = lax.rem, lax.div

    def place(zl=zl, x=x, zh=zh, y=y, k=k):
        return {"zl": zl, "x": x, "zh": zh, "y": y, "k": k}

    def at_column(j):
        return place(zh=div(j, 8), y=div(rem(j, 8), 2), k=rem(j, 2))

    def at_row(i):
        return place(zl=div(i, 4), x=rem(i, 4))

    def remote(src, dst, send_sem, recv_sem, where):
        return pltpu.make_async_remote_copy(
            src_ref=src, dst_ref=dst, send_sem=send_sem, recv_sem=recv_sem,
            device_id=where, device_id_type=MESH,
        )

    own_front = rem(c - r + 33, 8)
    own_slot = div(c - r - own_front + 1 + 64, 8) - 8
    owner = (own_front < FRONTS) & (own_slot >= 0) & (own_slot < N_SLOT)
    slot = jnp.clip(own_slot, 0, N_SLOT - 1)

    loads = [
        pltpu.make_async_copy(w_hbm, work, local.at[0]),
        pltpu.make_async_copy(a_hbm, a_all.at[1], local.at[1]),
        pltpu.make_async_copy(b_hbm, b_all.at[1], local.at[2]),
    ]
    factor_loads = [
        pltpu.make_async_copy(ia_hbm.at[slot], ia, local.at[3]),
        pltpu.make_async_copy(vb_hbm, vb, local.at[4]),
        pltpu.make_async_copy(va_hbm.at[slot], va, local.at[5]),
        pltpu.make_async_copy(ib_hbm, ib, local.at[6]),
    ]
    loads[0].start()

    @pl.when(owner)
    def _():
        for load in factor_loads:
            load.start()

    loads[1].start()
    loads[2].start()

    barrier = pltpu.get_barrier_semaphore()
    friends = [at_column(rem(c + by, N_COL)) for by in (1, 31, 2, 30, 3, 29)]
    friends += [at_row(rem(r + by, 8)) for by in range(1, 8)]
    friends += [place(k=1 - k)] + [place(y=rem(y + by, 4)) for by in (1, 2, 3)]
    friends += [place(zh=rem(zh + by, 4)) for by in (1, 2, 3)]
    for friend in friends:
        pl.semaphore_signal(barrier, inc=1, device_id=friend, device_id_type=MESH)

    @pl.when(owner)
    def _():
        left = jnp.concatenate(
            [la_ref[pl.ds(2 * slot, 1), :], la_ref[pl.ds(2 * slot + 1, 1), :]], axis=1
        )
        right = jnp.concatenate([lb_ref[pl.ds(0, 1), :], lb_ref[pl.ds(1, 1), :]], axis=1)
        denominator[...] = jnp.broadcast_to(left, (BLOCK, BLOCK)).T + right
        for load in factor_loads:
            load.wait()

    with jax.named_scope("barrier"):
        pl.semaphore_wait(barrier, len(friends))
    with jax.named_scope("loads"):
        for load in loads:
            load.wait()

    def block_of(ref, *index):
        return jnp.concatenate(
            [ref[(*index, pl.ds(0, BLOCK, 2), slice(None))], ref[(*index, pl.ds(1, BLOCK, 2), slice(None))]],
            axis=1,
        )

    def put_work(q, value):
        work[q, pl.ds(0, BLOCK, 2), :] = value[:, :HALF]
        work[q, pl.ds(1, BLOCK, 2), :] = value[:, HALF:]

    near_slot = div(c - 1 - r + 8, 8) - 1

    def shift_copies(q):
        above = 8 * q + r < c
        near = q == near_slot
        up_slot = jnp.minimum(q + div(r, 7), N_SLOT - 1)
        down_slot = jnp.maximum(q - jnp.where(r == 0, 1, 0), 0)
        yield True, above, remote(
            a_hbm.at[q], a_all.at[0, q], a_send.at[0, q], a_recv.at[0, q], at_column(jnp.maximum(c - 1, 0))
        )
        yield True, above, remote(
            b_hbm.at[q], b_all.at[0, up_slot], b_send.at[0, q], b_recv.at[0, up_slot], at_row(rem(r + 1, 8))
        )
        to_right = above & (c + 1 < N_COL)
        to_above = above & (8 * q + r > 0)
        right = remote(
            a_hbm.at[q], a_all.at[2, q], a_send.at[2, q], a_recv.at[2, q], at_column(jnp.minimum(c + 1, N_COL - 1))
        )
        higher = remote(
            b_hbm.at[q], b_all.at[2, down_slot], b_send.at[2, q], b_recv.at[2, down_slot], at_row(rem(r + 7, 8))
        )
        yield True, to_right & near, right
        yield True, to_above & near, higher
        yield False, to_right & jnp.logical_not(near), right
        yield False, to_above & jnp.logical_not(near), higher
        yield False, above & (c + 2 < N_COL) & (k == 0), remote(
            a_hbm.at[q], a_all.at[3, q], a_send.at[3, q], a_recv.at[3, q], at_column(jnp.minimum(c + 2, N_COL - 1))
        )

    def passed_copies(q):
        above = 8 * q + r + 1 < c
        down_slot = jnp.maximum(q - jnp.where(r == 0, 1, 0), 0)
        fresh = jnp.logical_not(owner & (own_front == 3) & (q == own_slot))
        here = 8 * q + r < c - 1
        yield here & fresh, here & (k == 0), remote(
            a_all.at[2, q], a_all.at[3, q], a_send.at[1, q], a_recv.at[3, q], place(k=1 - k)
        ), remote(a_all.at[2, q], a_all.at[2, q], a_send.at[2, q], a_recv.at[2, q], place(k=1 - k))
        yield above & fresh, above & (8 * q + r > 0), remote(
            b_all.at[2, q], b_all.at[3, down_slot], b_send.at[3, q], b_recv.at[3, down_slot], at_row(rem(r + 7, 8))
        ), remote(b_all.at[2, q], b_all.at[2, q], b_send.at[2, q], b_recv.at[2, q], at_row(rem(r + 7, 8)))

    def column_role(f):
        i0 = c - f + 1
        exists = (i0 >= 0) & (i0 < N_COL)
        r0 = rem(i0 + 8, 8)
        dx = rem(x - rem(r0, 4) + 4, 4)
        same = zl == div(r0, 4)
        return exists, dx, same

    def column_copies(f, t):
        exists, dx, same = column_role(f)
        half = x_col.at[f, pl.ds(t * HALF, HALF), :]

        def to(n, where):
            return remote(half, half, col_send.at[f, t, n], col_recv.at[f, t], where)

        source = exists & (dx == 0) & same
        twin = exists & (dx == 0) & jnp.logical_not(same) & (f < FRONTS - 1)
        yield source, to(3, place(zl=1 - zl))
        for by in (3, 1, 2):
            yield source | twin, to(by - 1, place(x=rem(x + by, 4)))
        for by in (3, 1, 2):
            yield source & (f == FRONTS - 1), to(3 + by, place(zl=1 - zl, x=rem(x + by, 4)))

    def column_arrival(f, t):
        exists, dx, same = column_role(f)
        half = x_col.at[f, pl.ds(t * HALF, HALF), :]
        source = (dx == 0) & same
        return exists & jnp.logical_not(source), remote(
            half, half, col_send.at[f, t, 0], col_recv.at[f, t], place(zl=1 - zl)
        )

    def row_role(f, q):
        total = r + f + 7
        place_in = rem(total, 8)
        plane = q + div(total, 8) - 1
        dy = rem(y - div(place_in, 2) + 4, 4)
        same = k == rem(place_in, 2)
        return plane, (plane >= 0) & (plane <= zh), dy, same

    def row_copies(f, q, t):
        plane, present, dy, same = row_role(f, q)
        half = x_row.at[f, q, pl.ds(t * HALF, HALF), :]

        def to(sem, where):
            return remote(half, half, sem, row_recv.at[f, q, t], where)

        carrier = present & same
        yield carrier, to(row_send.at[f, q, t, 0], place(k=1 - k))
        if t == 0:
            yield carrier & (dy != 3), to(row_send.at[f, q, t, 1], place(y=rem(y + 1, 4)))
        else:
            yield carrier & (dy != 1), to(row_send.at[f, q, t, 1], place(y=rem(y + 3, 4)))

    def far_copies(f, q, t):
        half = x_row.at[f, q, pl.ds(t * HALF, HALF), :]
        for by in (1, 2, 3):
            yield zh + by < 4, remote(
                half, half, row_far.at[t, by - 1], row_recv.at[f, q, t], place(zh=jnp.minimum(zh + by, 3))
            )

    def row_arrival(f, q, t):
        plane, present, dy, same = row_role(f, q)
        half = x_row.at[f, q, pl.ds(t * HALF, HALF), :]
        source = (plane == zh) & (dy == 0) & same
        return present & jnp.logical_not(source), remote(
            half, half, row_send.at[f, q, t, 0], row_recv.at[f, q, t], place(k=1 - k)
        )

    def start(condition, copy):
        @pl.when(condition)
        def _():
            copy.start()

    def drain(condition, copy):
        @pl.when(condition)
        def _():
            copy.wait_send()

    def land(condition, copy):
        @pl.when(condition)
        def _():
            copy.wait_recv()

    def subtract_upper(f, q, arrived, solved):
        land(arrived, remote(a_all.at[f, q], a_all.at[f, q], a_send.at[f, q], a_recv.at[f, q], place(k=1 - k)))
        put_work(q, block_of(work, q) - matmul(block_of(a_all, f, q), solved))

    def subtract_lower(f, q, arrived, solved):
        land(arrived, remote(b_all.at[f, q], b_all.at[f, q], b_send.at[f, q], b_recv.at[f, q], place(k=1 - k)))
        put_work(q, block_of(work, q) - matmul(solved, block_of(b_all, f, q)))

    def update(f, q):
        early = (f == 0) | (f == 3)

        @pl.when(c - f + 1 < N_COL)
        def _():
            subtract_upper(f, q, early, x_col[f])

        @pl.when(8 * q + r + f - 1 >= 0)
        def _():
            subtract_lower(f, q, early, x_row[f, q])

    def bulk(f):
        def one(q, carry):
            done_before = owner & (q == own_slot)

            @pl.when((c - 8 * q - r >= f) & jnp.logical_not(done_before))
            def _():
                update(f, q)

            return carry

        lax.fori_loop(0, N_SLOT, one, 0)

    def chain_copies(distances):
        i0 = 8 * own_slot + r
        for by in distances:
            later = own_front + by < FRONTS
            f = jnp.minimum(own_front, 2)
            yield later & (c + by < N_COL), remote(
                x_row.at[own_front, slot], chain_row.at[f], chain_send.at[0, by - 1], chain_recv.at[0, f],
                at_column(jnp.minimum(c + by, N_COL - 1)),
            )
            yield later & (i0 - by >= 0), remote(
                x_col.at[own_front], chain_col.at[f], chain_send.at[1, by - 1], chain_recv.at[1, f],
                at_row(rem(r + 8 - by, 8)),
            )

    def send_shifts(wanted):
        def one(step, carry):
            for first, condition, copy in shift_copies(N_SLOT - 1 - step):
                if first == wanted:
                    start(condition, copy)
            return carry

        lax.fori_loop(0, N_SLOT, one, 0)

    deferred = owner & (own_front < 2)
    send_shifts(True)

    @pl.when(jnp.logical_not(deferred))
    def _():
        send_shifts(False)

    @pl.when(owner)
    def _():
        def earlier(f, carry):
            @pl.when((f < own_front) & (c - f + 1 < N_COL))
            def _():
                with jax.named_scope("chain_col"):
                    land(True, remote(chain_col.at[f], chain_col.at[f], chain_send.at[1, 0], chain_recv.at[1, f], place(k=1 - k)))
                with jax.named_scope("chain_upper"):
                    subtract_upper(f, slot, f != 1, chain_col[f])

            @pl.when((f < own_front) & (8 * slot + r + f - 1 >= 0))
            def _():
                with jax.named_scope("chain_row"):
                    land(True, remote(chain_row.at[f], chain_row.at[f], chain_send.at[0, 0], chain_recv.at[0, f], place(k=1 - k)))
                with jax.named_scope("chain_lower"):
                    subtract_lower(f, slot, f != 1, chain_row[f])

            return carry

        lax.fori_loop(0, FRONTS - 1, earlier, 0)
        with jax.named_scope("solve"):
            rotated = matmul(matmul(ia[...], block_of(work, slot)), vb[...])
            solved = matmul(matmul(va[...], rotated / denominator[...]), ib[...])
            x_col[own_front] = solved
            x_row[own_front, slot] = solved
            put_work(slot, solved)
        for condition, copy in chain_copies((1,)):
            start(condition, copy)
        for t in (0, 1):
            for condition, copy in far_copies(own_front, slot, t):
                start(condition, copy)
        for t in (0, 1):
            for condition, copy in column_copies(own_front, t):
                start(condition, copy)
            for condition, copy in row_copies(own_front, slot, t):
                start(condition, copy)
        for condition, copy in chain_copies((2, 3)):
            start(condition, copy)

    @pl.when(deferred)
    def _():
        send_shifts(False)

    def receive_column(f):
        for t in (0, 1):
            arriving, arrival = column_arrival(f, t)

            @pl.when(arriving)
            def _():
                with jax.named_scope(f"col#t={t}"):
                    arrival.wait_recv()
                for condition, copy in column_copies(f, t):
                    start(condition, copy)

    distance = rem(c - r + 32, 8)
    relays_column = (distance >= 3) & (distance <= 5)

    @pl.when(relays_column)
    def _():
        receive_column(jnp.clip(distance - 3, 0, FRONTS - 1))

    mine = rem(k + r + 1, 2)

    def receive_row(f, q, t, wanted):
        arriving, arrival = row_arrival(f, q, t)

        @pl.when(arriving & wanted)
        def _():
            with jax.named_scope(f"row#t={t}"):
                arrival.wait_recv()
            for condition, copy in row_copies(f, q, t):
                start(condition, copy)

    def pass_on(step, carry):
        for arrived, forwarded, copy, arrival in passed_copies(N_SLOT - 1 - step):
            land(arrived, arrival)
            start(forwarded, copy)
        return carry

    def ring(n, carry):
        def one(step, carry):
            f = mine + 2 * div(step, N_SLOT)
            q = N_SLOT - 1 - rem(step, N_SLOT)
            _, _, dy, _ = row_role(f, q)
            receive_row(f, q, 0, dy == n)
            receive_row(f, q, 1, rem(4 - dy, 4) == n)
            return carry

        lax.fori_loop(0, 2 * N_SLOT, one, 0)

        @pl.when(n == 1)
        def _():
            with jax.named_scope("pass"):
                lax.fori_loop(0, N_SLOT, pass_on, 0)

        return carry

    lax.fori_loop(0, 4, ring, 0)

    def front(f, carry):
        @pl.when(jnp.logical_not(relays_column & (f == distance - 3)))
        def _():
            receive_column(f)

        def one(q, carry):
            for t in (0, 1):
                receive_row(f, q, t, rem(f, 2) != mine)
            return carry

        lax.fori_loop(0, N_SLOT, one, 0)
        with jax.named_scope("bulk"):
            bulk(f)
        return carry

    lax.fori_loop(0, FRONTS, front, 0)

    result = pltpu.make_async_copy(work, out_hbm, out_sem)
    result.start()

    def finish(q, carry):
        for _, condition, copy in shift_copies(q):
            drain(condition, copy)
        for _, forwarded, copy, _ in passed_copies(q):
            drain(forwarded, copy)
        return carry

    with jax.named_scope("finish"):
        lax.fori_loop(0, N_SLOT, finish, 0)

    def finish_front(f, carry):
        for t in (0, 1):
            for condition, copy in column_copies(f, t):
                drain(condition, copy)

        def one(q, carry):
            for t in (0, 1):
                for condition, copy in row_copies(f, q, t):
                    drain(condition, copy)
            return carry

        return lax.fori_loop(0, N_SLOT, one, carry)

    with jax.named_scope("finish_front"):
        lax.fori_loop(0, FRONTS, finish_front, 0)

    @pl.when(owner)
    def _():
        for condition, copy in chain_copies((1, 2, 3)):
            drain(condition, copy)
        for t in (0, 1):
            for condition, copy in far_copies(own_front, slot, t):
                drain(condition, copy)

    result.wait()


def body(
    upper_a, upper_b, right_side, vectors_a, inverse_a, values_a, vectors_b, inverse_b, values_b
):
    tall = (N_SLOT, 2 * BLOCK, HALF)
    square = (N_SLOT, BLOCK, BLOCK)
    anywhere = pl.BlockSpec(memory_space=pl.ANY)
    inside = pl.BlockSpec(memory_space=pltpu.VMEM)
    dma = pltpu.SemaphoreType.DMA
    solved = pl.pallas_call(
        kernel,
        out_shape=jax.ShapeDtypeStruct(tall, jnp.float32),
        in_specs=[anywhere] * 5 + [inside] + [anywhere] * 2 + [inside],
        out_specs=anywhere,
        scratch_shapes=[
            pltpu.VMEM((FRONTS, *tall), jnp.float32),
            pltpu.VMEM((FRONTS, *tall), jnp.float32),
            pltpu.VMEM(tall, jnp.float32),
            pltpu.VMEM(square, jnp.float32),
            pltpu.VMEM((FRONTS, *square), jnp.float32),
            *[pltpu.VMEM((FRONTS - 1, BLOCK, BLOCK), jnp.float32)] * 2,
            *[pltpu.VMEM((BLOCK, BLOCK), jnp.float32)] * 5,
            dma((4, N_SLOT)),
            dma((4, N_SLOT)),
            dma((4, N_SLOT)),
            dma((4, N_SLOT)),
            dma((FRONTS, N_SLOT, 2, 2)),
            dma((2, 3)),
            dma((FRONTS, N_SLOT, 2)),
            dma((FRONTS, 2, 7)),
            dma((FRONTS, 2)),
            dma((2, 3)),
            dma((2, 3)),
            dma((7,)),
            dma,
        ],
        compiler_params=pltpu.CompilerParams(
            collective_id=0, has_side_effects=True, vmem_limit_bytes=60 * 1024 * 1024
        ),
    )(
        upper_a.reshape(tall), upper_b.reshape(tall), right_side.reshape(tall),
        vectors_a.reshape(square), inverse_a.reshape(square), values_a.reshape(2 * N_SLOT, HALF),
        vectors_b.reshape(BLOCK, BLOCK), inverse_b.reshape(BLOCK, BLOCK), values_b.reshape(2, HALF),
    )
    return solved.reshape(right_side.shape)


def solution(mesh):
    finer = Mesh(mesh.devices.reshape(2, 4, 4, 4, 2), ROW + COL)
    whole = P(None, ROW, None, COL, None)
    placed = (
        whole, whole, whole,
        P(None, ROW, None, None), P(None, ROW, None, None), P(None, ROW, None),
        P(COL, None, None), P(COL, None, None), P(COL, None),
    )
    return jax.shard_map(body, mesh=finer, in_specs=placed, out_specs=whole, check_vma=False)
```

```python
import functools

import jax
import jax.numpy as jnp
from jax import lax
from jax.experimental import pallas as pl
from jax.experimental.pallas import tpu as pltpu
from jax.sharding import Mesh
from jax.sharding import PartitionSpec as P

FRONTS = 4
N_SLOT = 4
BLOCK = 256
HALF = 128
N_COL = 32
MESH = pl.DeviceIdType.MESH
ROW = ("zl", "x")
COL = ("zh", "y", "k")


def parts(value):
    high = value.astype(jnp.bfloat16)
    low = (value - high.astype(jnp.float32)).astype(jnp.bfloat16)
    return high, low


def matmul(former, latter):
    former_high, former_low = parts(former)
    latter_high, latter_low = parts(latter)
    left = jnp.concatenate([former_high, former_low, former_high], axis=1)
    right = jnp.concatenate([latter_high, latter_high, latter_low], axis=0)
    return jnp.dot(left, right, preferred_element_type=jnp.float32)


def kernel(
    a_hbm, b_hbm, w_hbm, va_hbm, ia_hbm, la_ref, vb_hbm, ib_hbm, lb_ref, out_hbm,
    a_all, b_all, work, x_col, x_row, chain_col, chain_row, va, ia, vb, ib, denominator,
    a_send, a_recv, b_send, b_recv, row_send, row_far, row_recv, col_send, col_recv, chain_send, chain_recv, local, out_sem,
):
    zl, x = lax.axis_index("zl"), lax.axis_index("x")
    zh, y, k = lax.axis_index("zh"), lax.axis_index("y"), lax.axis_index("k")
    r = zl * 4 + x
    c = zh * 8 + y * 2 + k
    rem, div = lax.rem, lax.div

    def place(zl=zl, x=x, zh=zh, y=y, k=k):
        return {"zl": zl, "x": x, "zh": zh, "y": y, "k": k}

    def at_column(j):
        return place(zh=div(j, 8), y=div(rem(j, 8), 2), k=rem(j, 2))

    def at_row(i):
        return place(zl=div(i, 4), x=rem(i, 4))

    def remote(src, dst, send_sem, recv_sem, where):
        return pltpu.make_async_remote_copy(
            src_ref=src, dst_ref=dst, send_sem=send_sem, recv_sem=recv_sem,
            device_id=where, device_id_type=MESH,
        )

    own_front = rem(c - r + 33, 8)
    own_slot = div(c - r - own_front + 1 + 64, 8) - 8
    owner = (own_front < FRONTS) & (own_slot >= 0) & (own_slot < N_SLOT)
    slot = jnp.clip(own_slot, 0, N_SLOT - 1)

    loads = [
        pltpu.make_async_copy(w_hbm, work, local.at[0]),
        pltpu.make_async_copy(a_hbm, a_all.at[1], local.at[1]),
        pltpu.make_async_copy(b_hbm, b_all.at[1], local.at[2]),
    ]
    factor_loads = [
        pltpu.make_async_copy(ia_hbm.at[slot], ia, local.at[3]),
        pltpu.make_async_copy(vb_hbm, vb, local.at[4]),
        pltpu.make_async_copy(va_hbm.at[slot], va, local.at[5]),
        pltpu.make_async_copy(ib_hbm, ib, local.at[6]),
    ]
    loads[0].start()

    @pl.when(owner)
    def _():
        for load in factor_loads:
            load.start()

    loads[1].start()
    loads[2].start()

    barrier = pltpu.get_barrier_semaphore()
    friends = [at_column(rem(c + by, N_COL)) for by in (1, 31, 2, 30)]
    friends += [at_row(rem(r + by, 8)) for by in range(1, 8)]
    friends += [place(k=1 - k)] + [place(y=rem(y + by, 4)) for by in (1, 2, 3)]
    friends += [place(zh=rem(zh + by, 4)) for by in (1, 2, 3)]
    for friend in friends:
        pl.semaphore_signal(barrier, inc=1, device_id=friend, device_id_type=MESH)

    @pl.when(owner)
    def _():
        left = jnp.concatenate(
            [la_ref[pl.ds(2 * slot, 1), :], la_ref[pl.ds(2 * slot + 1, 1), :]], axis=1
        )
        right = jnp.concatenate([lb_ref[pl.ds(0, 1), :], lb_ref[pl.ds(1, 1), :]], axis=1)
        denominator[...] = jnp.broadcast_to(left, (BLOCK, BLOCK)).T + right
        for load in factor_loads:
            load.wait()

    with jax.named_scope("barrier"):
        pl.semaphore_wait(barrier, len(friends))
    with jax.named_scope("loads"):
        for load in loads:
            load.wait()

    def block_of(ref, *index):
        return jnp.concatenate(
            [ref[(*index, pl.ds(0, BLOCK, 2), slice(None))], ref[(*index, pl.ds(1, BLOCK, 2), slice(None))]],
            axis=1,
        )

    def put_work(q, value):
        work[q, pl.ds(0, BLOCK, 2), :] = value[:, :HALF]
        work[q, pl.ds(1, BLOCK, 2), :] = value[:, HALF:]

    distance = rem(c - r + 32, 8)
    near_slot = div(c - 1 - r + 8, 8) - 1

    def shift_copies(q):
        above = 8 * q + r < c
        near = (q == near_slot) & (distance >= 1) & (distance <= 3)
        nearer = near & (distance == 1)
        crossing = (rem(c, 8) >= 6) & (x != 1)
        first_row = jnp.where(r == 0, 1, 0)
        second_row = jnp.where(r <= 1, 1, 0)
        left = at_column(jnp.maximum(c - 1, 0))
        right = at_column(jnp.minimum(c + 1, N_COL - 1))
        farther = at_column(jnp.minimum(c + 2, N_COL - 1))
        below, higher, highest = at_row(rem(r + 1, 8)), at_row(rem(r + 7, 8)), at_row(rem(r + 6, 8))

        def a_copy(f, where):
            return remote(a_hbm.at[q], a_all.at[f, q], a_send.at[f, q], a_recv.at[f, q], where)

        def b_copy(f, there, where):
            target = jnp.clip(there, 0, N_SLOT - 1)
            return remote(b_hbm.at[q], b_all.at[f, target], b_send.at[f, q], b_recv.at[f, target], where)

        sends = [
            (above, near, None, a_copy(0, left)),
            (above, near, None, b_copy(0, q + div(r, 7), below)),
            (above & (c + 1 < N_COL), nearer, crossing & (k == 1), a_copy(2, right)),
            (above & (8 * q + r >= 1), nearer, None, b_copy(2, q - first_row, higher)),
        ]
        for number, (wanted, soon, later, copy) in enumerate(sends):
            yield 0, wanted & soon, copy
            rest = wanted & jnp.logical_not(soon)
            if later is None:
                yield 4 if number < 2 else 1, rest, copy
            else:
                yield 1, rest & jnp.logical_not(later), copy
                yield 2, rest & later, copy
        wanted = above & (c + 2 < N_COL) & (k == 0)
        yield 1, wanted & jnp.logical_not(crossing), a_copy(3, farther)
        yield 2, wanted & crossing, a_copy(3, farther)
        yield 3, above & (8 * q + r >= 2), b_copy(3, q - second_row, highest)

    def passed_copy(q):
        fresh = jnp.logical_not(owner & (own_front == 3) & (q == own_slot))
        here = 8 * q + r < c - 1
        return here & fresh, here & (k == 0), remote(
            a_all.at[2, q], a_all.at[3, q], a_send.at[1, q], a_recv.at[3, q], place(k=1 - k)
        ), remote(a_all.at[2, q], a_all.at[2, q], a_send.at[2, q], a_recv.at[2, q], place(k=1 - k))

    def column_role(f):
        i0 = c - f + 1
        exists = (i0 >= 0) & (i0 < N_COL)
        r0 = rem(i0 + 8, 8)
        dx = rem(x - rem(r0, 4) + 4, 4)
        same = zl == div(r0, 4)
        return exists, dx, same

    def column_copies(f, t):
        exists, dx, same = column_role(f)
        half = x_col.at[f, pl.ds(t * HALF, HALF), :]

        def to(n, where):
            return remote(half, half, col_send.at[t, n], col_recv.at[f, t], where)

        source = exists & (dx == 0) & same
        twin = exists & (dx == 0) & jnp.logical_not(same) & (f < 2)
        yield source, to(3, place(zl=1 - zl))
        for by in (3, 1, 2):
            yield source | twin, to(by - 1, place(x=rem(x + by, 4)))
        for by in (3, 1, 2):
            yield source & (f >= 2), to(3 + by, place(zl=1 - zl, x=rem(x + by, 4)))

    def column_arrival(f, t):
        exists, dx, same = column_role(f)
        half = x_col.at[f, pl.ds(t * HALF, HALF), :]
        source = (dx == 0) & same
        return exists & jnp.logical_not(source), remote(
            half, half, col_send.at[t, 0], col_recv.at[f, t], place(zl=1 - zl)
        )

    def row_role(f, q):
        total = r + f + 7
        place_in = rem(total, 8)
        plane = q + div(total, 8) - 1
        dy = rem(y - div(place_in, 2) + 4, 4)
        same = k == rem(place_in, 2)
        return plane, (plane >= 0) & (plane <= zh), dy, same

    def row_copies(f, q, t):
        plane, present, dy, same = row_role(f, q)
        half = x_row.at[f, q, pl.ds(t * HALF, HALF), :]

        def to(sem, where):
            return remote(half, half, sem, row_recv.at[f, q, t], where)

        carrier = present & same
        yield carrier, to(row_send.at[div(f, 2), q, t, 0], place(k=1 - k))
        if t == 0:
            direct = f < 2
            yield carrier & ((dy == 0) | (dy == 2) | ((dy == 1) & jnp.logical_not(direct))), to(
                row_send.at[div(f, 2), q, t, 1], place(y=rem(y + 1, 4))
            )
            yield carrier & (dy == 0) & direct, to(row_send.at[div(f, 2), q, t, 2], place(y=rem(y + 2, 4)))
        else:
            yield carrier & (dy != 1), to(row_send.at[div(f, 2), q, t, 1], place(y=rem(y + 3, 4)))

    def far_copies(f, q, t):
        half = x_row.at[f, q, pl.ds(t * HALF, HALF), :]
        for by in (1, 2, 3):
            yield zh + by < 4, remote(
                half, half, row_far.at[t, by - 1], row_recv.at[f, q, t], place(zh=jnp.minimum(zh + by, 3))
            )

    def row_arrival(f, q, t):
        plane, present, dy, same = row_role(f, q)
        half = x_row.at[f, q, pl.ds(t * HALF, HALF), :]
        source = (plane == zh) & (dy == 0) & same
        return present & jnp.logical_not(source), remote(
            half, half, row_send.at[div(f, 2), q, t, 0], row_recv.at[f, q, t], place(k=1 - k)
        )

    def start(condition, copy):
        @pl.when(condition)
        def _():
            copy.start()

    def drain(condition, copy):
        @pl.when(condition)
        def _():
            copy.wait_send()

    def land(condition, copy):
        @pl.when(condition)
        def _():
            copy.wait_recv()

    def subtract_upper(f, q, arrived, solved):
        land(arrived, remote(a_all.at[f, q], a_all.at[f, q], a_send.at[f, q], a_recv.at[f, q], place(k=1 - k)))
        put_work(q, block_of(work, q) - matmul(block_of(a_all, f, q), solved))

    def subtract_lower(f, q, arrived, solved):
        land(arrived, remote(b_all.at[f, q], b_all.at[f, q], b_send.at[f, q], b_recv.at[f, q], place(k=1 - k)))
        put_work(q, block_of(work, q) - matmul(solved, block_of(b_all, f, q)))

    def update(f, q):

        @pl.when(c - f + 1 < N_COL)
        def _():
            subtract_upper(f, q, (f == 0) | (f == 3), x_col[f])

        @pl.when(8 * q + r + f - 1 >= 0)
        def _():
            subtract_lower(f, q, f != 1, x_row[f, q])

    def bulk(f, q):
        done_before = owner & (q == own_slot)

        @pl.when((c - 8 * q - r >= f) & jnp.logical_not(done_before))
        def _():
            update(f, q)

    def result(q):
        return pltpu.make_async_copy(work.at[q], out_hbm.at[q], out_sem.at[q])

    def chain_copies(f, row, column):
        wanted = owner & (own_front < FRONTS - 1)
        yield wanted & (c + 1 < N_COL), remote(
            row, chain_row.at[f], chain_send.at[0, f], chain_recv.at[0, f], at_column(jnp.minimum(c + 1, N_COL - 1))
        )
        yield wanted & (8 * own_slot + r > 0), remote(
            column, chain_col.at[f], chain_send.at[1, f], chain_recv.at[1, f], at_row(rem(r + 7, 8))
        )

    def relayed(f):
        return chain_copies(f, chain_row.at[f], chain_col.at[f])

    def own_copies():
        f = jnp.minimum(own_front, FRONTS - 2)
        return chain_copies(f, x_row.at[f, slot], x_col.at[f])

    def send_shifts(wanted):
        def one(step, carry):
            for first, condition, copy in shift_copies(N_SLOT - 1 - step):
                if first == wanted:
                    start(condition, copy)
            return carry

        lax.fori_loop(0, N_SLOT, one, 0)

    mine = rem(k + r + 1, 2)

    def receive_row(f, q, t, wanted):
        arriving, arrival = row_arrival(f, q, t)

        @pl.when(arriving & wanted)
        def _():
            with jax.named_scope(f"row#t={t}"):
                arrival.wait_recv()
            for condition, copy in row_copies(f, q, t):
                start(condition, copy)

    deferred = owner & (own_front < FRONTS - 1)
    last_deferred = deferred & (own_front < 2) & (rem(own_front + r, 2) == 1)
    beside_first = (distance == 6) & (rem(r, 2) == 0)
    nearest = jnp.clip(zh - div(r + 7, 8) + 1, 0, N_SLOT - 1)
    even_row = rem(r, 2) == 0
    after_arrival = (distance == 1) | (distance == 2) | ((distance == 0) & even_row)
    after_ring = (distance == 3) | ((distance == 4) & jnp.logical_not(even_row))
    send_shifts(0)

    @pl.when(jnp.logical_not(after_ring | (after_arrival & owner)))
    def _():
        send_shifts(4)

    @pl.when(beside_first)
    def _():
        for t in (0, 1):
            receive_row(0, nearest, t, True)

    @pl.when(jnp.logical_not(deferred))
    def _():
        send_shifts(1)

    @pl.when(owner)
    def _():
        row_first = ((k == 1) | (rem(r, 4) == 3)) & (rem(c, 8) != 0)

        def earlier(step, carry):
            f = div(step, 2)
            take_row = (rem(step, 2) == 0) == row_first

            @pl.when((f < own_front) & jnp.logical_not(take_row) & (c - f + 1 < N_COL))
            def _():
                with jax.named_scope("chain_col"):
                    land(True, remote(chain_col.at[f], chain_col.at[f], chain_send.at[1, 0], chain_recv.at[1, f], place(k=1 - k)))
                start(*list(relayed(f))[1])
                with jax.named_scope("chain_upper"):
                    subtract_upper(f, slot, f != 1, chain_col[f])

            @pl.when((f < own_front) & take_row & (8 * slot + r + f - 1 >= 0))
            def _():
                with jax.named_scope("chain_row"):
                    land(True, remote(chain_row.at[f], chain_row.at[f], chain_send.at[0, 0], chain_recv.at[0, f], place(k=1 - k)))
                start(*list(relayed(f))[0])
                with jax.named_scope("chain_lower"):
                    subtract_lower(f, slot, f != 1, chain_row[f])

            @pl.when(after_arrival & (step == 0))
            def _():
                send_shifts(4)

            return carry

        lax.fori_loop(0, 2 * (FRONTS - 1), earlier, 0)
        with jax.named_scope("solve"):
            rotated = matmul(matmul(ia[...], block_of(work, slot)), vb[...])
            solved = matmul(matmul(va[...], rotated / denominator[...]), ib[...])
            x_col[own_front] = solved
            x_row[own_front, slot] = solved
            put_work(slot, solved)
        for condition, copy in own_copies():
            start(condition, copy)
        for t in (0, 1):
            for condition, copy in far_copies(own_front, slot, t):
                start(condition, copy)
        for t in (0, 1):
            for condition, copy in column_copies(own_front, t):
                start(condition, copy)
            for condition, copy in row_copies(own_front, slot, t):
                start(condition, copy)

    @pl.when(deferred & jnp.logical_not(last_deferred))
    def _():
        send_shifts(1)

    @pl.when(owner)
    def _():
        send_shifts(2)

    def receive_column(f):
        for t in (0, 1):
            arriving, arrival = column_arrival(f, t)

            @pl.when(arriving)
            def _():
                with jax.named_scope(f"col#t={t}"):
                    arrival.wait_recv()
                for condition, copy in column_copies(f, t):
                    start(condition, copy)

    relays_column = (distance == 3) | (distance == 4)

    def pass_on(step, carry):
        arrived, forwarded, copy, arrival = passed_copy(N_SLOT - 1 - step)
        land(arrived, arrival)
        start(forwarded, copy)
        return carry

    def ring(f):
        def one(step, carry):
            n = div(step, N_SLOT)
            q = N_SLOT - 1 - rem(step, N_SLOT)
            _, _, dy, _ = row_role(f, q)
            receive_row(f, q, 0, dy == n)
            receive_row(f, q, 1, rem(4 - dy, 4) == n)
            return carry

        lax.fori_loop(0, 4 * N_SLOT, one, 0)

    late = (distance == 1) | (distance == 2)
    ring(jnp.where(late, mine + 2, mine))

    @pl.when(after_ring)
    def _():
        send_shifts(4)

    @pl.when(last_deferred)
    def _():
        send_shifts(1)

    @pl.when(jnp.logical_not(owner))
    def _():
        send_shifts(2)

    send_shifts(3)

    @pl.when(relays_column)
    def _():
        receive_column(distance - 3)

    ring(jnp.where(late, mine, mine + 2))
    with jax.named_scope("pass"):
        lax.fori_loop(0, N_SLOT, pass_on, 0)

    def front(f, carry):
        opening = f == 0

        @pl.when(jnp.logical_not(relays_column & (f == distance - 3)))
        def _():
            receive_column(f)

        def one(step, carry):
            q = N_SLOT - 1 - step
            leaf = (rem(f, 2) != mine) & jnp.logical_not(beside_first & opening & (q == nearest))
            for t in (0, 1):
                receive_row(f, q, t, leaf)
            with jax.named_scope("bulk"):
                bulk(f, q)

            @pl.when(f == FRONTS - 1)
            def _():
                result(q).start()

            return carry

        lax.fori_loop(0, N_SLOT, one, 0)
        return carry

    lax.fori_loop(0, FRONTS, front, 0)

    def finish(q, carry):
        for _, condition, copy in shift_copies(q):
            drain(condition, copy)
        _, forwarded, copy, _ = passed_copy(q)
        drain(forwarded, copy)
        return carry

    with jax.named_scope("finish"):
        lax.fori_loop(0, N_SLOT, finish, 0)

    def finish_front(f, carry):
        for t in (0, 1):
            for condition, copy in column_copies(f, t):
                drain(condition, copy)

        def one(q, carry):
            for t in (0, 1):
                for condition, copy in row_copies(f, q, t):
                    drain(condition, copy)
            return carry

        return lax.fori_loop(0, N_SLOT, one, carry)

    with jax.named_scope("finish_front"):
        lax.fori_loop(0, FRONTS, finish_front, 0)

    @pl.when(owner)
    def _():
        for condition, copy in own_copies():
            drain(condition, copy)

        def finish_chain(f, carry):
            beside, above = relayed(f)
            drain((f < own_front) & (8 * slot + r + f - 1 >= 0) & beside[0], beside[1])
            drain((f < own_front) & (c - f + 1 < N_COL) & above[0], above[1])
            return carry

        lax.fori_loop(0, FRONTS - 1, finish_chain, 0)
        for t in (0, 1):
            for condition, copy in far_copies(own_front, slot, t):
                drain(condition, copy)

    for q in range(N_SLOT):
        result(q).wait()


def body(
    upper_a, upper_b, right_side, vectors_a, inverse_a, values_a, vectors_b, inverse_b, values_b
):
    tall = (N_SLOT, 2 * BLOCK, HALF)
    square = (N_SLOT, BLOCK, BLOCK)
    anywhere = pl.BlockSpec(memory_space=pl.ANY)
    inside = pl.BlockSpec(memory_space=pltpu.VMEM)
    dma = pltpu.SemaphoreType.DMA
    solved = pl.pallas_call(
        kernel,
        out_shape=jax.ShapeDtypeStruct(tall, jnp.float32),
        in_specs=[anywhere] * 5 + [inside] + [anywhere] * 2 + [inside],
        out_specs=anywhere,
        scratch_shapes=[
            pltpu.VMEM((FRONTS, *tall), jnp.float32),
            pltpu.VMEM((FRONTS, *tall), jnp.float32),
            pltpu.VMEM(tall, jnp.float32),
            pltpu.VMEM(square, jnp.float32),
            pltpu.VMEM((FRONTS, *square), jnp.float32),
            *[pltpu.VMEM((FRONTS - 1, BLOCK, BLOCK), jnp.float32)] * 2,
            *[pltpu.VMEM((BLOCK, BLOCK), jnp.float32)] * 5,
            dma((4, N_SLOT)),
            dma((4, N_SLOT)),
            dma((4, N_SLOT)),
            dma((4, N_SLOT)),
            dma((FRONTS // 2, N_SLOT, 2, 3)),
            dma((2, 3)),
            dma((FRONTS, N_SLOT, 2)),
            dma((2, 7)),
            dma((FRONTS, 2)),
            dma((2, 3)),
            dma((2, 3)),
            dma((7,)),
            dma((N_SLOT,)),
        ],
        compiler_params=pltpu.CompilerParams(
            collective_id=0, has_side_effects=True, vmem_limit_bytes=60 * 1024 * 1024
        ),
    )(
        upper_a.reshape(tall), upper_b.reshape(tall), right_side.reshape(tall),
        vectors_a.reshape(square), inverse_a.reshape(square), values_a.reshape(2 * N_SLOT, HALF),
        vectors_b.reshape(BLOCK, BLOCK), inverse_b.reshape(BLOCK, BLOCK), values_b.reshape(2, HALF),
    )
    return solved.reshape(right_side.shape)


def solution(mesh):
    finer = Mesh(mesh.devices.reshape(2, 4, 4, 4, 2), ROW + COL)
    whole = P(None, ROW, None, COL, None)
    placed = (
        whole, whole, whole,
        P(None, ROW, None, None), P(None, ROW, None, None), P(None, ROW, None),
        P(COL, None, None), P(COL, None, None), P(COL, None),
    )
    return jax.shard_map(body, mesh=finer, in_specs=placed, out_specs=whole, check_vma=False)
```

```python
import functools

import jax
import jax.numpy as jnp
from jax import lax
from jax.experimental import pallas as pl
from jax.experimental.pallas import tpu as pltpu
from jax.sharding import Mesh
from jax.sharding import PartitionSpec as P

FRONTS = 4
N_SLOT = 4
BLOCK = 256
HALF = 128
N_COL = 32
MESH = pl.DeviceIdType.MESH
ROW = ("zl", "x")
COL = ("zh", "y", "k")


def parts(value):
    high = value.astype(jnp.bfloat16)
    low = (value - high.astype(jnp.float32)).astype(jnp.bfloat16)
    return high, low


def matmul(former, latter):
    former_high, former_low = parts(former)
    latter_high, latter_low = parts(latter)
    left = jnp.concatenate([former_high, former_low, former_high], axis=1)
    right = jnp.concatenate([latter_high, latter_high, latter_low], axis=0)
    return jnp.dot(left, right, preferred_element_type=jnp.float32)


def kernel(
    a_hbm, b_hbm, w_hbm, va_hbm, ia_hbm, la_ref, vb_hbm, ib_hbm, lb_ref, work,
    a_all, b_all, x_col, x_row, chain_col, chain_row, va, ia, vb, ib, denominator,
    a_send, a_recv, b_send, b_recv, row_send, row_far, row_recv, col_send, col_recv, chain_send, chain_recv, local,
):
    zl, x = lax.axis_index("zl"), lax.axis_index("x")
    zh, y, k = lax.axis_index("zh"), lax.axis_index("y"), lax.axis_index("k")
    r = zl * 4 + x
    c = zh * 8 + y * 2 + k
    rem, div = lax.rem, lax.div

    def place(zl=zl, x=x, zh=zh, y=y, k=k):
        return {"zl": zl, "x": x, "zh": zh, "y": y, "k": k}

    def at_column(j):
        return place(zh=div(j, 8), y=div(rem(j, 8), 2), k=rem(j, 2))

    def at_row(i):
        return place(zl=div(i, 4), x=rem(i, 4))

    def remote(src, dst, send_sem, recv_sem, where):
        return pltpu.make_async_remote_copy(
            src_ref=src, dst_ref=dst, send_sem=send_sem, recv_sem=recv_sem,
            device_id=where, device_id_type=MESH,
        )

    own_front = rem(c - r + 33, 8)
    own_slot = div(c - r - own_front + 1 + 64, 8) - 8
    owner = (own_front < FRONTS) & (own_slot >= 0) & (own_slot < N_SLOT)
    slot = jnp.clip(own_slot, 0, N_SLOT - 1)

    loads = [
        pltpu.make_async_copy(w_hbm, work, local.at[0]),
        pltpu.make_async_copy(a_hbm, a_all.at[1], local.at[1]),
        pltpu.make_async_copy(b_hbm, b_all.at[1], local.at[2]),
    ]
    factor_loads = [
        pltpu.make_async_copy(ia_hbm.at[slot], ia, local.at[3]),
        pltpu.make_async_copy(vb_hbm, vb, local.at[4]),
        pltpu.make_async_copy(va_hbm.at[slot], va, local.at[5]),
        pltpu.make_async_copy(ib_hbm, ib, local.at[6]),
    ]
    loads[0].start()

    @pl.when(owner)
    def _():
        for load in factor_loads:
            load.start()

    loads[1].start()
    loads[2].start()

    barrier = pltpu.get_barrier_semaphore()
    friends = [at_column(rem(c + by, N_COL)) for by in (1, 31, 2, 30)]
    friends += [at_row(rem(r + by, 8)) for by in range(1, 8)]
    friends += [place(k=1 - k)] + [place(y=rem(y + by, 4)) for by in (1, 2, 3)]
    friends += [place(zh=rem(zh + by, 4)) for by in (1, 2, 3)]
    for friend in friends:
        pl.semaphore_signal(barrier, inc=1, device_id=friend, device_id_type=MESH)

    @pl.when(owner)
    def _():
        left = jnp.concatenate(
            [la_ref[pl.ds(2 * slot, 1), :], la_ref[pl.ds(2 * slot + 1, 1), :]], axis=1
        )
        right = jnp.concatenate([lb_ref[pl.ds(0, 1), :], lb_ref[pl.ds(1, 1), :]], axis=1)
        denominator[...] = jnp.broadcast_to(left, (BLOCK, BLOCK)).T + right
        for load in factor_loads:
            load.wait()

    with jax.named_scope("barrier"):
        pl.semaphore_wait(barrier, len(friends))
    with jax.named_scope("loads"):
        for load in loads:
            load.wait()

    def block_of(ref, *index):
        return jnp.concatenate(
            [ref[(*index, pl.ds(0, BLOCK, 2), slice(None))], ref[(*index, pl.ds(1, BLOCK, 2), slice(None))]],
            axis=1,
        )

    def put_work(q, value):
        work[q, pl.ds(0, BLOCK, 2), :] = value[:, :HALF]
        work[q, pl.ds(1, BLOCK, 2), :] = value[:, HALF:]

    distance = rem(c - r + 32, 8)
    near_slot = div(c - 1 - r + 8, 8) - 1

    def shift_copies(q):
        above = 8 * q + r < c
        near = (q == near_slot) & (distance >= 1) & (distance <= 3)
        nearer = near & (distance == 1)
        crossing = (rem(c, 8) >= 6) & (x != 1) & ((x == 0) | (zl == 1))
        first_row = jnp.where(r == 0, 1, 0)
        second_row = jnp.where(r <= 1, 1, 0)
        left = at_column(jnp.maximum(c - 1, 0))
        right = at_column(jnp.minimum(c + 1, N_COL - 1))
        farther = at_column(jnp.minimum(c + 2, N_COL - 1))
        below, higher, highest = at_row(rem(r + 1, 8)), at_row(rem(r + 7, 8)), at_row(rem(r + 6, 8))

        def a_copy(f, where):
            return remote(a_hbm.at[q], a_all.at[f, q], a_send.at[f, q], a_recv.at[f, q], where)

        def b_copy(f, there, where):
            target = jnp.clip(there, 0, N_SLOT - 1)
            return remote(b_hbm.at[q], b_all.at[f, target], b_send.at[f, q], b_recv.at[f, target], where)

        sends = [
            (above, near, None, a_copy(0, left)),
            (above, near, None, b_copy(0, q + div(r, 7), below)),
            (above & (c + 1 < N_COL), nearer, crossing & (k == 1), a_copy(2, right)),
            (above & (8 * q + r >= 1), nearer, None, b_copy(2, q - first_row, higher)),
        ]
        for number, (wanted, soon, later, copy) in enumerate(sends):
            yield 0, wanted & soon, copy
            rest = wanted & jnp.logical_not(soon)
            if later is None:
                yield 4 if number < 2 else 1, rest, copy
            else:
                yield 1, rest & jnp.logical_not(later), copy
                yield 2, rest & later, copy
        wanted = above & (c + 2 < N_COL) & (k == 0)
        yield 1, wanted & jnp.logical_not(crossing), a_copy(3, farther)
        yield 2, wanted & crossing, a_copy(3, farther)
        yield 3, above & (x >= 2), b_copy(3, q - second_row, highest)

    def passed_copy(q):
        fresh = jnp.logical_not(owner & (own_front == 3) & (q == own_slot))
        here = 8 * q + r < c - 1
        return here & fresh, here & (k == 0), remote(
            a_all.at[2, q], a_all.at[3, q], a_send.at[1, q], a_recv.at[3, q], place(k=1 - k)
        ), remote(a_all.at[2, q], a_all.at[2, q], a_send.at[2, q], a_recv.at[2, q], place(k=1 - k))

    hands_on = (x == 0) | (x == 3)

    def handed_copy(q):
        fresh = jnp.logical_not(owner & (own_front == 3) & (q == own_slot))
        here = hands_on & (8 * q + r + 1 < c)
        down_slot = jnp.maximum(q - jnp.where(r == 0, 1, 0), 0)
        return here & fresh, here & (8 * q + r > 0), remote(
            b_all.at[2, q], b_all.at[3, down_slot], b_send.at[1, q], b_recv.at[3, down_slot], at_row(rem(r + 7, 8))
        ), remote(b_all.at[2, q], b_all.at[2, q], b_send.at[2, q], b_recv.at[2, q], place(k=1 - k))

    def column_role(f):
        i0 = c - f + 1
        exists = (i0 >= 0) & (i0 < N_COL)
        r0 = rem(i0 + 8, 8)
        dx = rem(x - rem(r0, 4) + 4, 4)
        same = zl == div(r0, 4)
        return exists, dx, same

    def column_copies(f, t):
        exists, dx, same = column_role(f)
        half = x_col.at[f, pl.ds(t * HALF, HALF), :]

        def to(n, where):
            return remote(half, half, col_send.at[t, n], col_recv.at[f, t], where)

        source = exists & (dx == 0) & same
        yield source, to(3, place(zl=1 - zl))
        for by in (3, 1, 2):
            yield source, to(by - 1, place(x=rem(x + by, 4)))
        for by in (3, 1, 2):
            yield source, to(3 + by, place(zl=1 - zl, x=rem(x + by, 4)))

    def column_arrival(f, t):
        exists, dx, same = column_role(f)
        half = x_col.at[f, pl.ds(t * HALF, HALF), :]
        source = (dx == 0) & same
        return exists & jnp.logical_not(source), remote(
            half, half, col_send.at[t, 0], col_recv.at[f, t], place(zl=1 - zl)
        )

    def row_role(f, q):
        total = r + f + 7
        place_in = rem(total, 8)
        plane = q + div(total, 8) - 1
        dy = rem(y - div(place_in, 2) + 4, 4)
        same = k == rem(place_in, 2)
        return plane, (plane >= 0) & (plane <= zh), dy, same

    def row_copies(f, q, t):
        plane, present, dy, same = row_role(f, q)
        half = x_row.at[f, q, pl.ds(t * HALF, HALF), :]

        def to(sem, where):
            return remote(half, half, sem, row_recv.at[f, q, t], where)

        carrier = present & same
        yield carrier, to(row_send.at[div(f, 2), q, t, 0], place(k=1 - k))
        if t == 0:
            direct = f < 2
            yield carrier & ((dy == 0) | (dy == 2) | ((dy == 1) & jnp.logical_not(direct))), to(
                row_send.at[div(f, 2), q, t, 1], place(y=rem(y + 1, 4))
            )
            yield carrier & (dy == 0) & direct, to(row_send.at[div(f, 2), q, t, 2], place(y=rem(y + 2, 4)))
        else:
            yield carrier & (dy != 1), to(row_send.at[div(f, 2), q, t, 1], place(y=rem(y + 3, 4)))

    def far_copies(f, q, t):
        half = x_row.at[f, q, pl.ds(t * HALF, HALF), :]
        for by in (1, 2, 3):
            yield zh + by < 4, remote(
                half, half, row_far.at[t, by - 1], row_recv.at[f, q, t], place(zh=jnp.minimum(zh + by, 3))
            )

    def row_arrival(f, q, t):
        plane, present, dy, same = row_role(f, q)
        half = x_row.at[f, q, pl.ds(t * HALF, HALF), :]
        source = (plane == zh) & (dy == 0) & same
        return present & jnp.logical_not(source), remote(
            half, half, row_send.at[div(f, 2), q, t, 0], row_recv.at[f, q, t], place(k=1 - k)
        )

    def start(condition, copy):
        @pl.when(condition)
        def _():
            copy.start()

    def drain(condition, copy):
        @pl.when(condition)
        def _():
            copy.wait_send()

    def land(condition, copy):
        @pl.when(condition)
        def _():
            copy.wait_recv()

    def land_a(f, q, wanted):
        land(wanted, remote(a_all.at[f, q], a_all.at[f, q], a_send.at[f, q], a_recv.at[f, q], place(k=1 - k)))

    def land_b(f, q, wanted):
        land(wanted, remote(b_all.at[f, q], b_all.at[f, q], b_send.at[f, q], b_recv.at[f, q], place(k=1 - k)))

    def subtract_upper(f, q, solved):
        put_work(q, block_of(work, q) - matmul(block_of(a_all, f, q), solved))

    def subtract_lower(f, q, solved):
        put_work(q, block_of(work, q) - matmul(solved, block_of(b_all, f, q)))

    def update(f, q):
        ahead = c - 8 * q - r
        open_block = jnp.logical_not(owner & (q == own_slot))
        upper = c - f + 1 < N_COL
        lower = 8 * q + r + f - 1 >= 0
        both = open_block & (ahead >= f + 1) & upper & lower
        for g, pending in ((f, open_block & (ahead >= f)), (f + 1, open_block & (ahead >= f + 1))):
            land_a(g, q, pending & (c - g + 1 < N_COL) & ((g == 0) | (g == 3)))
            land_b(
                g, q, pending & (8 * q + r + g - 1 >= 0) & ((g == 0) | (g == 3) | ((g == 2) & jnp.logical_not(hands_on)))
            )

        @pl.when(both)
        def _():
            left = jnp.concatenate(
                [block_of(a_all, f, q), block_of(a_all, f + 1, q), x_row[f, q], x_row[f + 1, q]], axis=1
            )
            right = jnp.concatenate(
                [x_col[f], x_col[f + 1], block_of(b_all, f, q), block_of(b_all, f + 1, q)], axis=0
            )
            put_work(q, block_of(work, q) - matmul(left, right))

        def one(g, carry):
            pending = open_block & jnp.logical_not(both) & (ahead >= g)

            @pl.when(pending & (c - g + 1 < N_COL))
            def _():
                subtract_upper(g, q, x_col[g])

            @pl.when(pending & (8 * q + r + g - 1 >= 0))
            def _():
                subtract_lower(g, q, x_row[g, q])

            return carry

        lax.fori_loop(f, f + 2, one, 0)

    def chain_copies(f, row, column):
        wanted = owner & (own_front < FRONTS - 1)
        yield wanted & (c + 1 < N_COL), remote(
            row, chain_row.at[f], chain_send.at[0, f], chain_recv.at[0, f], at_column(jnp.minimum(c + 1, N_COL - 1))
        )
        yield wanted & (8 * own_slot + r > 0), remote(
            column, chain_col.at[f], chain_send.at[1, f], chain_recv.at[1, f], at_row(rem(r + 7, 8))
        )

    def relayed(f):
        return chain_copies(f, chain_row.at[f], chain_col.at[f])

    def own_copies():
        f = jnp.minimum(own_front, FRONTS - 2)
        return chain_copies(f, x_row.at[f, slot], x_col.at[f])

    def send_shifts(wanted):
        def one(step, carry):
            for first, condition, copy in shift_copies(N_SLOT - 1 - step):
                if first == wanted:
                    start(condition, copy)
            return carry

        lax.fori_loop(0, N_SLOT, one, 0)

    mine = rem(k + r + 1, 2)

    def receive_row(f, q, t, wanted):
        arriving, arrival = row_arrival(f, q, t)

        @pl.when(arriving & wanted)
        def _():
            with jax.named_scope(f"row#t={t}"):
                arrival.wait_recv()
            for condition, copy in row_copies(f, q, t):
                start(condition, copy)

    deferred = owner & (own_front < FRONTS - 1)
    even_row = rem(r, 2) == 0
    after_arrival = owner & ((distance == 1) | (distance == 2) | ((distance == 0) & even_row))
    fourth = (distance == 4) & (k == 1)
    beside = ((k == 0) & ((distance == 6) | (distance == 7) | (distance == 0))) | fourth
    beside_front = jnp.where(beside & jnp.logical_not(fourth), rem(distance + 2, 8), 0)
    nearest = zh - div(r + beside_front + 7, 8) + 1
    watches = beside & (nearest >= 0) & (nearest < N_SLOT)
    watched = jnp.clip(nearest, 0, N_SLOT - 1)

    def watch():
        for t in (0, 1):
            receive_row(beside_front, watched, t, True)

    solves_later = (distance == 7) | (distance == 0)
    send_shifts(0)

    @pl.when(jnp.logical_not(after_arrival | fourth))
    def _():
        send_shifts(4)

    @pl.when(watches & jnp.logical_not(solves_later))
    def _():
        watch()

    @pl.when(fourth)
    def _():
        send_shifts(4)

    middle = (distance >= 3) & (distance <= 5)

    @pl.when(jnp.logical_not(deferred))
    def _():
        send_shifts(1)

    @pl.when(middle)
    def _():
        send_shifts(3)

    @pl.when(owner)
    def _():
        row_first = ((k == 1) | (rem(r, 4) == 3)) & (rem(c, 8) != 0)

        def earlier(step, carry):
            f = div(step, 2)
            take_row = (rem(step, 2) == 0) == row_first

            @pl.when((f < own_front) & jnp.logical_not(take_row) & (c - f + 1 < N_COL))
            def _():
                with jax.named_scope("chain_col"):
                    land(True, remote(chain_col.at[f], chain_col.at[f], chain_send.at[1, 0], chain_recv.at[1, f], place(k=1 - k)))
                start(*list(relayed(f))[1])
                with jax.named_scope("chain_upper"):
                    land_a(f, slot, f != 1)
                    subtract_upper(f, slot, chain_col[f])

            @pl.when((f < own_front) & take_row & (8 * slot + r + f - 1 >= 0))
            def _():
                with jax.named_scope("chain_row"):
                    land(True, remote(chain_row.at[f], chain_row.at[f], chain_send.at[0, 0], chain_recv.at[0, f], place(k=1 - k)))
                start(*list(relayed(f))[0])
                with jax.named_scope("chain_lower"):
                    land_b(f, slot, f != 1)
                    subtract_lower(f, slot, chain_row[f])

            @pl.when(after_arrival & (step == 0))
            def _():
                send_shifts(4)

            return carry

        lax.fori_loop(0, 2 * (FRONTS - 1), earlier, 0)
        with jax.named_scope("solve"):
            rotated = matmul(matmul(ia[...], block_of(work, slot)), vb[...])
            solved = matmul(matmul(va[...], rotated / denominator[...]), ib[...])
            x_col[own_front] = solved
            x_row[own_front, slot] = solved
            put_work(slot, solved)
        for condition, copy in own_copies():
            start(condition, copy)
        for t in (0, 1):
            for condition, copy in far_copies(own_front, slot, t):
                start(condition, copy)
        for t in (0, 1):
            for condition, copy in column_copies(own_front, t):
                start(condition, copy)
            for condition, copy in row_copies(own_front, slot, t):
                start(condition, copy)

    @pl.when(watches & solves_later)
    def _():
        watch()

    @pl.when(deferred)
    def _():
        send_shifts(1)

    @pl.when(owner)
    def _():
        send_shifts(2)

    @pl.when(jnp.logical_not(middle))
    def _():
        send_shifts(3)

    def receive_column(f):
        for t in (0, 1):
            with jax.named_scope(f"col#t={t}"):
                land(*column_arrival(f, t))

    def pass_on(which):
        def one(step, carry):
            arrived, forwarded, copy, arrival = which(N_SLOT - 1 - step)
            land(arrived, arrival)
            start(forwarded, copy)
            return carry

        with jax.named_scope("pass"):
            lax.fori_loop(0, N_SLOT, one, 0)

    def ring(f):
        def one(step, carry):
            n = div(step, N_SLOT)
            q = N_SLOT - 1 - rem(step, N_SLOT)
            _, _, dy, _ = row_role(f, q)
            receive_row(f, q, 0, dy == n)
            receive_row(f, q, 1, rem(4 - dy, 4) == n)
            return carry

        lax.fori_loop(0, 4 * N_SLOT, one, 0)

    late = (distance == 1) | (distance == 2)
    ring(jnp.where(late, mine + 2, mine))

    @pl.when(jnp.logical_not(owner))
    def _():
        send_shifts(2)

    pass_on(handed_copy)

    def pair(f):
        for g in (f, f + 1):
            receive_column(g)

        def one(step, carry):
            q = N_SLOT - 1 - step
            for g in (f, f + 1):
                leaf = (rem(g, 2) != mine) & jnp.logical_not(watches & (g == beside_front) & (q == nearest))
                for t in (0, 1):
                    receive_row(g, q, t, leaf)
            with jax.named_scope("bulk"):
                update(f, q)
            return carry

        lax.fori_loop(0, N_SLOT, one, 0)

    early = (mine == 1) & ((distance == 0) | (distance >= 4)) & (x != 0) & (rem(c, 8) != 7)

    def stage(j, carry):
        @pl.when(j == 1)
        def _():
            ring(jnp.where(late, mine, mine + 2))
            pass_on(passed_copy)

        @pl.when((j == 3) | ((j == 0) & early) | ((j == 2) & jnp.logical_not(early)))
        def _():
            pair(jnp.where(j == 3, 2, 0))

        return carry

    lax.fori_loop(0, 4, stage, 0)

    def finish(q, carry):
        for _, condition, copy in shift_copies(q):
            drain(condition, copy)
        for _, forwarded, copy, _ in (passed_copy(q), handed_copy(q)):
            drain(forwarded, copy)
        return carry

    with jax.named_scope("finish"):
        lax.fori_loop(0, N_SLOT, finish, 0)

    def finish_front(f, carry):
        for t in (0, 1):
            for condition, copy in column_copies(f, t):
                drain(condition, copy)

        def one(q, carry):
            for t in (0, 1):
                for condition, copy in row_copies(f, q, t):
                    drain(condition, copy)
            return carry

        return lax.fori_loop(0, N_SLOT, one, carry)

    with jax.named_scope("finish_front"):
        lax.fori_loop(0, FRONTS, finish_front, 0)

    @pl.when(owner)
    def _():
        for condition, copy in own_copies():
            drain(condition, copy)

        def finish_chain(f, carry):
            beside, above = relayed(f)
            drain((f < own_front) & (8 * slot + r + f - 1 >= 0) & beside[0], beside[1])
            drain((f < own_front) & (c - f + 1 < N_COL) & above[0], above[1])
            return carry

        lax.fori_loop(0, FRONTS - 1, finish_chain, 0)
        for t in (0, 1):
            for condition, copy in far_copies(own_front, slot, t):
                drain(condition, copy)


def body(
    upper_a, upper_b, right_side, vectors_a, inverse_a, values_a, vectors_b, inverse_b, values_b
):
    tall = (N_SLOT, 2 * BLOCK, HALF)
    square = (N_SLOT, BLOCK, BLOCK)
    anywhere = pl.BlockSpec(memory_space=pl.ANY)
    inside = pl.BlockSpec(memory_space=pltpu.VMEM)
    dma = pltpu.SemaphoreType.DMA
    solved = pl.pallas_call(
        kernel,
        out_shape=pltpu.VMEM(tall, jnp.float32),
        in_specs=[anywhere] * 5 + [inside] + [anywhere] * 2 + [inside],
        out_specs=inside,
        scratch_shapes=[
            pltpu.VMEM((FRONTS, *tall), jnp.float32),
            pltpu.VMEM((FRONTS, *tall), jnp.float32),
            pltpu.VMEM(square, jnp.float32),
            pltpu.VMEM((FRONTS, *square), jnp.float32),
            *[pltpu.VMEM((FRONTS - 1, BLOCK, BLOCK), jnp.float32)] * 2,
            *[pltpu.VMEM((BLOCK, BLOCK), jnp.float32)] * 5,
            dma((4, N_SLOT)),
            dma((4, N_SLOT)),
            dma((4, N_SLOT)),
            dma((4, N_SLOT)),
            dma((FRONTS // 2, N_SLOT, 2, 3)),
            dma((2, 3)),
            dma((FRONTS, N_SLOT, 2)),
            dma((2, 7)),
            dma((FRONTS, 2)),
            dma((2, 3)),
            dma((2, 3)),
            dma((7,)),
        ],
        compiler_params=pltpu.CompilerParams(
            collective_id=0, has_side_effects=True, vmem_limit_bytes=60 * 1024 * 1024
        ),
    )(
        upper_a.reshape(tall), upper_b.reshape(tall), right_side.reshape(tall),
        vectors_a.reshape(square), inverse_a.reshape(square), values_a.reshape(2 * N_SLOT, HALF),
        vectors_b.reshape(BLOCK, BLOCK), inverse_b.reshape(BLOCK, BLOCK), values_b.reshape(2, HALF),
    )
    return solved.reshape(right_side.shape)


def solution(mesh):
    finer = Mesh(mesh.devices.reshape(2, 4, 4, 4, 2), ROW + COL)
    whole = P(None, ROW, None, COL, None)
    placed = (
        whole, whole, whole,
        P(None, ROW, None, None), P(None, ROW, None, None), P(None, ROW, None),
        P(COL, None, None), P(COL, None, None), P(COL, None),
    )
    return jax.shard_map(body, mesh=finer, in_specs=placed, out_specs=whole, check_vma=False)
```

```python
import functools

import jax
import jax.numpy as jnp
from jax import lax
from jax.experimental import pallas as pl
from jax.experimental.pallas import tpu as pltpu
from jax.sharding import Mesh
from jax.sharding import PartitionSpec as P

FRONTS = 4
N_SLOT = 4
BLOCK = 256
HALF = 128
N_COL = 32
MESH = pl.DeviceIdType.MESH
ROW = ("zl", "x")
COL = ("zh", "y", "k")


def parts(value):
    high = value.astype(jnp.bfloat16)
    low = (value - high.astype(jnp.float32)).astype(jnp.bfloat16)
    return high, low


def matmul(former, latter):
    former_high, former_low = parts(former)
    latter_high, latter_low = parts(latter)
    left = jnp.concatenate([former_high, former_low, former_high], axis=1)
    right = jnp.concatenate([latter_high, latter_high, latter_low], axis=0)
    return jnp.dot(left, right, preferred_element_type=jnp.float32)


def kernel(
    a_hbm, b_hbm, w_hbm, va_hbm, ia_hbm, la_ref, vb_hbm, ib_hbm, lb_ref, work,
    a_all, b_all, x_col, x_row, chain_row, va, ia, vb, ib, denominator,
    a_send, a_recv, b_send, b_recv, row_send, row_far, row_recv, col_send, col_recv, chain_send, chain_recv, local,
):
    zl, x = lax.axis_index("zl"), lax.axis_index("x")
    zh, y, k = lax.axis_index("zh"), lax.axis_index("y"), lax.axis_index("k")
    r = zl * 4 + x
    c = zh * 8 + y * 2 + k
    rem, div = lax.rem, lax.div

    def place(zl=zl, x=x, zh=zh, y=y, k=k):
        return {"zl": zl, "x": x, "zh": zh, "y": y, "k": k}

    def at_column(j):
        return place(zh=div(j, 8), y=div(rem(j, 8), 2), k=rem(j, 2))

    def at_row(i):
        return place(zl=div(i, 4), x=rem(i, 4))

    def remote(src, dst, send_sem, recv_sem, where):
        return pltpu.make_async_remote_copy(
            src_ref=src, dst_ref=dst, send_sem=send_sem, recv_sem=recv_sem,
            device_id=where, device_id_type=MESH,
        )

    own_front = rem(c - r + 33, 8)
    own_slot = div(c - r - own_front + 1 + 64, 8) - 8
    owner = (own_front < FRONTS) & (own_slot >= 0) & (own_slot < N_SLOT)
    slot = jnp.clip(own_slot, 0, N_SLOT - 1)

    loads = [
        pltpu.make_async_copy(w_hbm, work, local.at[0]),
        pltpu.make_async_copy(a_hbm, a_all.at[1], local.at[1]),
        pltpu.make_async_copy(b_hbm, b_all.at[1], local.at[2]),
    ]
    factor_loads = [
        pltpu.make_async_copy(ia_hbm.at[slot], ia, local.at[3]),
        pltpu.make_async_copy(vb_hbm, vb, local.at[4]),
        pltpu.make_async_copy(va_hbm.at[slot], va, local.at[5]),
        pltpu.make_async_copy(ib_hbm, ib, local.at[6]),
    ]
    loads[0].start()

    @pl.when(owner)
    def _():
        for load in factor_loads:
            load.start()

    loads[1].start()
    loads[2].start()

    barrier = pltpu.get_barrier_semaphore()
    friends = [at_column(rem(c + by, N_COL)) for by in (1, 31, 2, 30)]
    friends += [at_row(rem(r + by, 8)) for by in range(1, 8)]
    friends += [place(k=1 - k)] + [place(y=rem(y + by, 4)) for by in (1, 2, 3)]
    friends += [place(zh=rem(zh + by, 4)) for by in (1, 2, 3)]
    for friend in friends:
        pl.semaphore_signal(barrier, inc=1, device_id=friend, device_id_type=MESH)

    @pl.when(owner)
    def _():
        left = jnp.concatenate(
            [la_ref[pl.ds(2 * slot, 1), :], la_ref[pl.ds(2 * slot + 1, 1), :]], axis=1
        )
        right = jnp.concatenate([lb_ref[pl.ds(0, 1), :], lb_ref[pl.ds(1, 1), :]], axis=1)
        denominator[...] = jnp.broadcast_to(left, (BLOCK, BLOCK)).T + right
        for load in factor_loads:
            load.wait()

    with jax.named_scope("barrier"):
        pl.semaphore_wait(barrier, len(friends))
    with jax.named_scope("loads"):
        for load in loads:
            load.wait()

    def block_of(ref, *index):
        return jnp.concatenate(
            [ref[(*index, pl.ds(0, BLOCK, 2), slice(None))], ref[(*index, pl.ds(1, BLOCK, 2), slice(None))]],
            axis=1,
        )

    def put_work(q, value):
        work[q, pl.ds(0, BLOCK, 2), :] = value[:, :HALF]
        work[q, pl.ds(1, BLOCK, 2), :] = value[:, HALF:]

    distance = rem(c - r + 32, 8)
    near_slot = div(c - 1 - r + 8, 8) - 1

    def shift_copies(q):
        above = 8 * q + r < c
        near = (q == near_slot) & (distance >= 1) & (distance <= 3)
        nearer = near & (distance == 1)
        crossing = (rem(c, 8) >= 6) & (x != 1) & ((x == 0) | (zl == 1))
        first_row = jnp.where(r == 0, 1, 0)
        second_row = jnp.where(r <= 1, 1, 0)
        left = at_column(jnp.maximum(c - 1, 0))
        right = at_column(jnp.minimum(c + 1, N_COL - 1))
        farther = at_column(jnp.minimum(c + 2, N_COL - 1))
        below, higher, highest = at_row(rem(r + 1, 8)), at_row(rem(r + 7, 8)), at_row(rem(r + 6, 8))

        def a_copy(f, where):
            return remote(a_hbm.at[q], a_all.at[f, q], a_send.at[f, q], a_recv.at[f, q], where)

        def b_copy(f, there, where):
            target = jnp.clip(there, 0, N_SLOT - 1)
            return remote(b_hbm.at[q], b_all.at[f, target], b_send.at[f, q], b_recv.at[f, target], where)

        sends = [
            (above, near, None, a_copy(0, left)),
            (above, near, None, b_copy(0, q + div(r, 7), below)),
            (above & (c + 1 < N_COL), nearer, crossing & (k == 1), a_copy(2, right)),
            (above & (8 * q + r >= 1), nearer, None, b_copy(2, q - first_row, higher)),
        ]
        for number, (wanted, soon, later, copy) in enumerate(sends):
            yield 0, wanted & soon, copy
            rest = wanted & jnp.logical_not(soon)
            if later is None:
                yield 4 if number < 2 else 1, rest, copy
            else:
                yield 1, rest & jnp.logical_not(later), copy
                yield 2, rest & later, copy
        wanted = above & (c + 2 < N_COL) & (k == 0)
        yield 1, wanted & jnp.logical_not(crossing), a_copy(3, farther)
        yield 2, wanted & crossing, a_copy(3, farther)
        yield 3, above & (x >= 2), b_copy(3, q - second_row, highest)

    def passed_copy(q):
        fresh = jnp.logical_not(owner & (own_front == 3) & (q == own_slot))
        here = 8 * q + r < c - 1
        return here & fresh, here & (k == 0), remote(
            a_all.at[2, q], a_all.at[3, q], a_send.at[1, q], a_recv.at[3, q], place(k=1 - k)
        ), remote(a_all.at[2, q], a_all.at[2, q], a_send.at[2, q], a_recv.at[2, q], place(k=1 - k))

    hands_on = (x == 0) | (x == 3)

    def handed_copy(q):
        fresh = jnp.logical_not(owner & (own_front == 3) & (q == own_slot))
        here = hands_on & (8 * q + r + 1 < c)
        down_slot = jnp.maximum(q - jnp.where(r == 0, 1, 0), 0)
        return here & fresh, here & (8 * q + r > 0), remote(
            b_all.at[2, q], b_all.at[3, down_slot], b_send.at[1, q], b_recv.at[3, down_slot], at_row(rem(r + 7, 8))
        ), remote(b_all.at[2, q], b_all.at[2, q], b_send.at[2, q], b_recv.at[2, q], place(k=1 - k))

    def column_role(f):
        i0 = c - f + 1
        exists = (i0 >= 0) & (i0 < N_COL)
        r0 = rem(i0 + 8, 8)
        dx = rem(x - rem(r0, 4) + 4, 4)
        same = zl == div(r0, 4)
        return exists, dx, same

    def column_copies(f, t):
        exists, dx, same = column_role(f)
        half = x_col.at[f, pl.ds(t * HALF, HALF), :]

        def to(n, where):
            return remote(half, half, col_send.at[t, n], col_recv.at[f, t], where)

        source = exists & (dx == 0) & same
        for n in range(7):
            there_zl = zl if n < 3 else 1 - zl
            there_x = rem(x + (3, 1, 2, 0, 3, 1, 2)[n], 4)
            apart = rem(r - there_zl * 4 - there_x + 8, 8)
            chained = (apart <= FRONTS - 1 - f) & (c - f + 1 - apart >= 0)
            yield source & jnp.logical_not(chained), to(n, place(zl=there_zl, x=there_x))

    def column_arrival(f, t):
        exists, dx, same = column_role(f)
        half = x_col.at[f, pl.ds(t * HALF, HALF), :]
        source = (dx == 0) & same
        return exists & jnp.logical_not(source | (owner & (own_front > f))), remote(
            half, half, col_send.at[t, 0], col_recv.at[f, t], place(zl=1 - zl)
        )

    def row_role(f, q):
        total = r + f + 7
        place_in = rem(total, 8)
        plane = q + div(total, 8) - 1
        dy = rem(y - div(place_in, 2) + 4, 4)
        same = k == rem(place_in, 2)
        return plane, (plane >= 0) & (plane <= zh), dy, same

    def row_copies(f, q, t):
        plane, present, dy, same = row_role(f, q)
        half = x_row.at[f, q, pl.ds(t * HALF, HALF), :]

        def to(sem, where):
            return remote(half, half, sem, row_recv.at[f, q, t], where)

        carrier = present & same
        yield carrier, to(row_send.at[div(f, 2), q, t, 0], place(k=1 - k))
        if t == 0:
            direct = f < 2
            yield carrier & ((dy == 0) | (dy == 2) | ((dy == 1) & jnp.logical_not(direct))), to(
                row_send.at[div(f, 2), q, t, 1], place(y=rem(y + 1, 4))
            )
            yield carrier & (dy == 0) & direct, to(row_send.at[div(f, 2), q, t, 2], place(y=rem(y + 2, 4)))
        else:
            yield carrier & (dy != 1), to(row_send.at[div(f, 2), q, t, 1], place(y=rem(y + 3, 4)))

    def far_copies(f, q, t):
        half = x_row.at[f, q, pl.ds(t * HALF, HALF), :]
        for by in (1, 2, 3):
            yield zh + by < 4, remote(
                half, half, row_far.at[t, by - 1], row_recv.at[f, q, t], place(zh=jnp.minimum(zh + by, 3))
            )

    def row_arrival(f, q, t):
        plane, present, dy, same = row_role(f, q)
        half = x_row.at[f, q, pl.ds(t * HALF, HALF), :]
        source = (plane == zh) & (dy == 0) & same
        return present & jnp.logical_not(source), remote(
            half, half, row_send.at[div(f, 2), q, t, 0], row_recv.at[f, q, t], place(k=1 - k)
        )

    def start(condition, copy):
        @pl.when(condition)
        def _():
            copy.start()

    def drain(condition, copy):
        @pl.when(condition)
        def _():
            copy.wait_send()

    def land(condition, copy):
        @pl.when(condition)
        def _():
            copy.wait_recv()

    def land_a(f, q, wanted):
        land(wanted, remote(a_all.at[f, q], a_all.at[f, q], a_send.at[f, q], a_recv.at[f, q], place(k=1 - k)))

    def land_b(f, q, wanted):
        land(wanted, remote(b_all.at[f, q], b_all.at[f, q], b_send.at[f, q], b_recv.at[f, q], place(k=1 - k)))

    def subtract_upper(f, q, solved):
        put_work(q, block_of(work, q) - matmul(block_of(a_all, f, q), solved))

    def subtract_lower(f, q, solved):
        put_work(q, block_of(work, q) - matmul(solved, block_of(b_all, f, q)))

    def update(f, q):
        ahead = c - 8 * q - r
        open_block = jnp.logical_not(owner & (q == own_slot))
        upper = c - f + 1 < N_COL
        lower = 8 * q + r + f - 1 >= 0
        both = open_block & (ahead >= f + 1) & upper & lower
        for g, pending in ((f, open_block & (ahead >= f)), (f + 1, open_block & (ahead >= f + 1))):
            land_a(g, q, pending & (c - g + 1 < N_COL) & ((g == 0) | (g == 3)))
            land_b(
                g, q, pending & (8 * q + r + g - 1 >= 0) & ((g == 0) | (g == 3) | ((g == 2) & jnp.logical_not(hands_on)))
            )

        @pl.when(both)
        def _():
            left = jnp.concatenate(
                [block_of(a_all, f, q), block_of(a_all, f + 1, q), x_row[f, q], x_row[f + 1, q]], axis=1
            )
            right = jnp.concatenate(
                [x_col[f], x_col[f + 1], block_of(b_all, f, q), block_of(b_all, f + 1, q)], axis=0
            )
            put_work(q, block_of(work, q) - matmul(left, right))

        def one(g, carry):
            pending = open_block & jnp.logical_not(both) & (ahead >= g)

            @pl.when(pending & (c - g + 1 < N_COL))
            def _():
                subtract_upper(g, q, x_col[g])

            @pl.when(pending & (8 * q + r + g - 1 >= 0))
            def _():
                subtract_lower(g, q, x_row[g, q])

            return carry

        lax.fori_loop(f, f + 2, one, 0)

    def chain_copies(f, row, column):
        wanted = owner & (own_front < FRONTS - 1)
        yield wanted & (c + 1 < N_COL), remote(
            row, chain_row.at[f], chain_send.at[0, f], chain_recv.at[0, f], at_column(jnp.minimum(c + 1, N_COL - 1))
        )
        yield wanted & (8 * own_slot + r > 0), remote(
            column, x_col.at[f], chain_send.at[1, f], chain_recv.at[1, f], at_row(rem(r + 7, 8))
        )

    def relayed(f):
        return chain_copies(f, chain_row.at[f], x_col.at[f])

    def own_copies():
        f = jnp.minimum(own_front, FRONTS - 2)
        return chain_copies(f, x_row.at[f, slot], x_col.at[f])

    def send_shifts(wanted):
        def one(step, carry):
            for first, condition, copy in shift_copies(N_SLOT - 1 - step):
                if first == wanted:
                    start(condition, copy)
            return carry

        lax.fori_loop(0, N_SLOT, one, 0)

    mine = rem(k + r + 1, 2)

    def receive_row(f, q, t, wanted):
        arriving, arrival = row_arrival(f, q, t)

        @pl.when(arriving & wanted)
        def _():
            with jax.named_scope(f"row#t={t}"):
                arrival.wait_recv()
            for condition, copy in row_copies(f, q, t):
                start(condition, copy)

    deferred = owner & (own_front < FRONTS - 1)
    even_row = rem(r, 2) == 0
    after_arrival = owner & ((distance == 1) | (distance == 2) | ((distance == 0) & even_row))
    fourth = (distance == 4) & (k == 1)
    beside = ((k == 0) & ((distance == 6) | (distance == 7) | ((distance == 0) & (x != 0)))) | fourth
    beside_front = jnp.where(beside & jnp.logical_not(fourth), rem(distance + 2, 8), 0)
    nearest = zh - div(r + beside_front + 7, 8) + 1
    watches = beside & (nearest >= 0) & (nearest < N_SLOT)
    watched = jnp.clip(nearest, 0, N_SLOT - 1)

    def watch():
        for t in (0, 1):
            receive_row(beside_front, watched, t, True)

    solves_later = (distance == 7) | (distance == 0)
    send_shifts(0)

    @pl.when(jnp.logical_not(after_arrival | fourth))
    def _():
        send_shifts(4)

    @pl.when(watches & jnp.logical_not(solves_later))
    def _():
        watch()

    @pl.when(fourth)
    def _():
        send_shifts(4)

    middle = (distance >= 3) & (distance <= 5)

    @pl.when(jnp.logical_not(deferred))
    def _():
        send_shifts(1)

    @pl.when(middle)
    def _():
        send_shifts(3)

    @pl.when(owner)
    def _():
        row_first = ((k == 1) | (rem(r, 4) == 3)) & (rem(c, 8) != 0)

        def earlier(step, carry):
            f = div(step, 2)
            take_row = (rem(step, 2) == 0) == row_first

            @pl.when((f < own_front) & jnp.logical_not(take_row) & (c - f + 1 < N_COL))
            def _():
                with jax.named_scope("chain_col"):
                    land(True, remote(x_col.at[f], x_col.at[f], chain_send.at[1, 0], chain_recv.at[1, f], place(k=1 - k)))
                start(*list(relayed(f))[1])
                with jax.named_scope("chain_upper"):
                    land_a(f, slot, f != 1)
                    subtract_upper(f, slot, x_col[f])

            @pl.when((f < own_front) & take_row & (8 * slot + r + f - 1 >= 0))
            def _():
                with jax.named_scope("chain_row"):
                    land(True, remote(chain_row.at[f], chain_row.at[f], chain_send.at[0, 0], chain_recv.at[0, f], place(k=1 - k)))
                start(*list(relayed(f))[0])
                with jax.named_scope("chain_lower"):
                    land_b(f, slot, f != 1)
                    subtract_lower(f, slot, chain_row[f])

            @pl.when(after_arrival & (step == 0))
            def _():
                send_shifts(4)

            return carry

        lax.fori_loop(0, 2 * (FRONTS - 1), earlier, 0)
        with jax.named_scope("solve"):
            rotated = matmul(matmul(ia[...], block_of(work, slot)), vb[...])
            solved = matmul(matmul(va[...], rotated / denominator[...]), ib[...])
            x_col[own_front] = solved
            x_row[own_front, slot] = solved
            put_work(slot, solved)
        for condition, copy in own_copies():
            start(condition, copy)
        for t in (0, 1):
            for condition, copy in far_copies(own_front, slot, t):
                start(condition, copy)
        for t in (0, 1):
            for condition, copy in column_copies(own_front, t):
                start(condition, copy)
            for condition, copy in row_copies(own_front, slot, t):
                start(condition, copy)

    @pl.when(watches & solves_later)
    def _():
        watch()

    @pl.when(deferred)
    def _():
        send_shifts(1)

    @pl.when(owner)
    def _():
        send_shifts(2)

    @pl.when(jnp.logical_not(middle))
    def _():
        send_shifts(3)

    def receive_column(f):
        for t in (0, 1):
            with jax.named_scope(f"col#t={t}"):
                land(*column_arrival(f, t))

    def pass_on(which):
        def one(step, carry):
            arrived, forwarded, copy, arrival = which(N_SLOT - 1 - step)
            land(arrived, arrival)
            start(forwarded, copy)
            return carry

        with jax.named_scope("pass"):
            lax.fori_loop(0, N_SLOT, one, 0)

    def ring(f):
        def one(step, carry):
            n = div(step, N_SLOT)
            q = N_SLOT - 1 - rem(step, N_SLOT)
            _, _, dy, _ = row_role(f, q)
            receive_row(f, q, 0, dy == n)
            receive_row(f, q, 1, rem(4 - dy, 4) == n)
            return carry

        lax.fori_loop(0, 4 * N_SLOT, one, 0)

    late = (distance == 1) | (distance == 2)
    ring(jnp.where(late, mine + 2, mine))

    @pl.when(jnp.logical_not(owner))
    def _():
        send_shifts(2)

    pass_on(handed_copy)

    def pair(f):
        for g in (f, f + 1):
            receive_column(g)

        def one(step, carry):
            q = N_SLOT - 1 - step
            for g in (f, f + 1):
                leaf = (rem(g, 2) != mine) & jnp.logical_not(watches & (g == beside_front) & (q == nearest))
                for t in (0, 1):
                    receive_row(g, q, t, leaf)
            with jax.named_scope("bulk"):
                update(f, q)
            return carry

        lax.fori_loop(0, N_SLOT, one, 0)

    early = (mine == 1) & ((distance == 0) | (distance >= 4)) & (x != 0) & (rem(c, 8) != 7)

    def stage(j, carry):
        @pl.when(j == 1)
        def _():
            ring(jnp.where(late, mine, mine + 2))
            pass_on(passed_copy)

        @pl.when((j == 3) | ((j == 0) & early) | ((j == 2) & jnp.logical_not(early)))
        def _():
            pair(jnp.where(j == 3, 2, 0))

        return carry

    lax.fori_loop(0, 4, stage, 0)

    def finish(q, carry):
        for _, condition, copy in shift_copies(q):
            drain(condition, copy)
        for _, forwarded, copy, _ in (passed_copy(q), handed_copy(q)):
            drain(forwarded, copy)
        return carry

    with jax.named_scope("finish"):
        lax.fori_loop(0, N_SLOT, finish, 0)

    def finish_front(f, carry):
        for t in (0, 1):
            for condition, copy in column_copies(f, t):
                drain(condition, copy)

        def one(q, carry):
            for t in (0, 1):
                for condition, copy in row_copies(f, q, t):
                    drain(condition, copy)
            return carry

        return lax.fori_loop(0, N_SLOT, one, carry)

    with jax.named_scope("finish_front"):
        lax.fori_loop(0, FRONTS, finish_front, 0)

    @pl.when(owner)
    def _():
        for condition, copy in own_copies():
            drain(condition, copy)

        def finish_chain(f, carry):
            beside, above = relayed(f)
            drain((f < own_front) & (8 * slot + r + f - 1 >= 0) & beside[0], beside[1])
            drain((f < own_front) & (c - f + 1 < N_COL) & above[0], above[1])
            return carry

        lax.fori_loop(0, FRONTS - 1, finish_chain, 0)
        for t in (0, 1):
            for condition, copy in far_copies(own_front, slot, t):
                drain(condition, copy)


def body(
    upper_a, upper_b, right_side, vectors_a, inverse_a, values_a, vectors_b, inverse_b, values_b
):
    tall = (N_SLOT, 2 * BLOCK, HALF)
    square = (N_SLOT, BLOCK, BLOCK)
    anywhere = pl.BlockSpec(memory_space=pl.ANY)
    inside = pl.BlockSpec(memory_space=pltpu.VMEM)
    dma = pltpu.SemaphoreType.DMA
    solved = pl.pallas_call(
        kernel,
        out_shape=pltpu.VMEM(tall, jnp.float32),
        in_specs=[anywhere] * 5 + [inside] + [anywhere] * 2 + [inside],
        out_specs=inside,
        scratch_shapes=[
            pltpu.VMEM((FRONTS, *tall), jnp.float32),
            pltpu.VMEM((FRONTS, *tall), jnp.float32),
            pltpu.VMEM(square, jnp.float32),
            pltpu.VMEM((FRONTS, *square), jnp.float32),
            pltpu.VMEM((FRONTS - 1, BLOCK, BLOCK), jnp.float32),
            *[pltpu.VMEM((BLOCK, BLOCK), jnp.float32)] * 5,
            dma((4, N_SLOT)),
            dma((4, N_SLOT)),
            dma((4, N_SLOT)),
            dma((4, N_SLOT)),
            dma((FRONTS // 2, N_SLOT, 2, 3)),
            dma((2, 3)),
            dma((FRONTS, N_SLOT, 2)),
            dma((2, 7)),
            dma((FRONTS, 2)),
            dma((2, 3)),
            dma((2, 3)),
            dma((7,)),
        ],
        compiler_params=pltpu.CompilerParams(
            collective_id=0, has_side_effects=True, vmem_limit_bytes=60 * 1024 * 1024
        ),
    )(
        upper_a.reshape(tall), upper_b.reshape(tall), right_side.reshape(tall),
        vectors_a.reshape(square), inverse_a.reshape(square), values_a.reshape(2 * N_SLOT, HALF),
        vectors_b.reshape(BLOCK, BLOCK), inverse_b.reshape(BLOCK, BLOCK), values_b.reshape(2, HALF),
    )
    return solved.reshape(right_side.shape)


def solution(mesh):
    finer = Mesh(mesh.devices.reshape(2, 4, 4, 4, 2), ROW + COL)
    whole = P(None, ROW, None, COL, None)
    placed = (
        whole, whole, whole,
        P(None, ROW, None, None), P(None, ROW, None, None), P(None, ROW, None),
        P(COL, None, None), P(COL, None, None), P(COL, None),
    )
    return jax.shard_map(body, mesh=finer, in_specs=placed, out_specs=whole, check_vma=False)
```

```python
import functools

import jax
import jax.numpy as jnp
from jax import lax
from jax.experimental import pallas as pl
from jax.experimental.pallas import tpu as pltpu
from jax.sharding import Mesh
from jax.sharding import PartitionSpec as P

FRONTS = 4
N_SLOT = 4
BLOCK = 256
HALF = 128
N_COL = 32
MESH = pl.DeviceIdType.MESH
ROW = ("zl", "x")
COL = ("zh", "y", "k")


def parts(value):
    high = value.astype(jnp.bfloat16)
    low = (value - high.astype(jnp.float32)).astype(jnp.bfloat16)
    return high, low


def matmul(former, latter):
    former_high, former_low = parts(former)
    latter_high, latter_low = parts(latter)
    left = jnp.concatenate([former_high, former_low, former_high], axis=1)
    right = jnp.concatenate([latter_high, latter_high, latter_low], axis=0)
    return jnp.dot(left, right, preferred_element_type=jnp.float32)


def kernel(
    a_hbm, b_hbm, w_hbm, va_hbm, ia_hbm, la_ref, vb_hbm, ib_hbm, lb_ref, work,
    a_all, b_all, x_col, x_row, chain_row, va, ia, vb, ib, denominator,
    a_send, a_recv, b_send, b_recv, row_send, row_far, row_recv, col_send, col_recv, chain_send, chain_recv, local,
):
    zl, x = lax.axis_index("zl"), lax.axis_index("x")
    zh, y, k = lax.axis_index("zh"), lax.axis_index("y"), lax.axis_index("k")
    r = zl * 4 + x
    c = zh * 8 + y * 2 + k
    rem, div = lax.rem, lax.div

    def place(zl=zl, x=x, zh=zh, y=y, k=k):
        return {"zl": zl, "x": x, "zh": zh, "y": y, "k": k}

    def at_column(j):
        return place(zh=div(j, 8), y=div(rem(j, 8), 2), k=rem(j, 2))

    def at_row(i):
        return place(zl=div(i, 4), x=rem(i, 4))

    def remote(src, dst, send_sem, recv_sem, where):
        return pltpu.make_async_remote_copy(
            src_ref=src, dst_ref=dst, send_sem=send_sem, recv_sem=recv_sem,
            device_id=where, device_id_type=MESH,
        )

    own_front = rem(c - r + 33, 8)
    own_slot = div(c - r - own_front + 1 + 64, 8) - 8
    owner = (own_front < FRONTS) & (own_slot >= 0) & (own_slot < N_SLOT)
    slot = jnp.clip(own_slot, 0, N_SLOT - 1)

    loads = [
        pltpu.make_async_copy(w_hbm, work, local.at[0]),
        pltpu.make_async_copy(a_hbm, a_all.at[1], local.at[1]),
        pltpu.make_async_copy(b_hbm, b_all.at[1], local.at[2]),
    ]
    factor_loads = [
        pltpu.make_async_copy(ia_hbm.at[slot], ia, local.at[3]),
        pltpu.make_async_copy(vb_hbm, vb, local.at[4]),
        pltpu.make_async_copy(va_hbm.at[slot], va, local.at[5]),
        pltpu.make_async_copy(ib_hbm, ib, local.at[6]),
    ]
    loads[0].start()

    @pl.when(owner)
    def _():
        for load in factor_loads:
            load.start()

    loads[1].start()
    loads[2].start()

    barrier = pltpu.get_barrier_semaphore()
    friends = [at_column(rem(c + by, N_COL)) for by in (1, 31, 2, 30)]
    friends += [at_row(rem(r + by, 8)) for by in range(1, 8)]
    friends += [place(k=1 - k)] + [place(y=rem(y + by, 4)) for by in (1, 2, 3)]
    friends += [place(zh=rem(zh + by, 4)) for by in (1, 2, 3)]
    for friend in friends:
        pl.semaphore_signal(barrier, inc=1, device_id=friend, device_id_type=MESH)

    @pl.when(owner)
    def _():
        left = jnp.concatenate(
            [la_ref[pl.ds(2 * slot, 1), :], la_ref[pl.ds(2 * slot + 1, 1), :]], axis=1
        )
        right = jnp.concatenate([lb_ref[pl.ds(0, 1), :], lb_ref[pl.ds(1, 1), :]], axis=1)
        denominator[...] = jnp.broadcast_to(left, (BLOCK, BLOCK)).T + right
        for load in factor_loads:
            load.wait()

    with jax.named_scope("barrier"):
        pl.semaphore_wait(barrier, len(friends))
    with jax.named_scope("loads"):
        for load in loads:
            load.wait()

    def block_of(ref, *index):
        return jnp.concatenate(
            [ref[(*index, pl.ds(0, BLOCK, 2), slice(None))], ref[(*index, pl.ds(1, BLOCK, 2), slice(None))]],
            axis=1,
        )

    def put_work(q, value):
        work[q, pl.ds(0, BLOCK, 2), :] = value[:, :HALF]
        work[q, pl.ds(1, BLOCK, 2), :] = value[:, HALF:]

    distance = rem(c - r + 32, 8)
    near_slot = div(c - 1 - r + 8, 8) - 1

    def shift_copies(q):
        above = 8 * q + r < c
        near = (q == near_slot) & (distance >= 1) & (distance <= 3)
        nearer = near & (distance == 1)
        crossing = (rem(c, 8) >= 6) & (x != 1) & ((x == 0) | (zl == 1))
        first_row = jnp.where(r == 0, 1, 0)
        second_row = jnp.where(r <= 1, 1, 0)
        left = at_column(jnp.maximum(c - 1, 0))
        right = at_column(jnp.minimum(c + 1, N_COL - 1))
        farther = at_column(jnp.minimum(c + 2, N_COL - 1))
        below, higher, highest = at_row(rem(r + 1, 8)), at_row(rem(r + 7, 8)), at_row(rem(r + 6, 8))

        def a_copy(f, where):
            return remote(a_hbm.at[q], a_all.at[f, q], a_send.at[f, q], a_recv.at[f, q], where)

        def b_copy(f, there, where):
            target = jnp.clip(there, 0, N_SLOT - 1)
            return remote(b_hbm.at[q], b_all.at[f, target], b_send.at[f, q], b_recv.at[f, target], where)

        sends = [
            (above, near, None, a_copy(0, left)),
            (above, near, None, b_copy(0, q + div(r, 7), below)),
            (above & (c + 1 < N_COL), nearer, crossing & (k == 1), a_copy(2, right)),
            (above & (8 * q + r >= 1), nearer, None, b_copy(2, q - first_row, higher)),
        ]
        for number, (wanted, soon, later, copy) in enumerate(sends):
            yield 0, wanted & soon, copy
            rest = wanted & jnp.logical_not(soon)
            if later is None:
                yield 4 if number < 2 else 1, rest, copy
            else:
                yield 1, rest & jnp.logical_not(later), copy
                yield 2, rest & later, copy
        wanted = above & (c + 2 < N_COL) & (k == 0)
        yield 1, wanted & jnp.logical_not(crossing), a_copy(3, farther)
        yield 2, wanted & crossing, a_copy(3, farther)
        yield 3, above & (x == 2), b_copy(3, q - second_row, highest)

    def passed_copy(q):
        fresh = jnp.logical_not(owner & (own_front == 3) & (q == own_slot))
        here = 8 * q + r < c - 1
        return here & fresh, here & (k == 0), remote(
            a_all.at[2, q], a_all.at[3, q], a_send.at[1, q], a_recv.at[3, q], place(k=1 - k)
        ), remote(a_all.at[2, q], a_all.at[2, q], a_send.at[2, q], a_recv.at[2, q], place(k=1 - k))

    hands_on = x != 1

    def handed_copy(q):
        fresh = jnp.logical_not(owner & (own_front == 3) & (q == own_slot))
        here = hands_on & (8 * q + r + 1 < c)
        down_slot = jnp.maximum(q - jnp.where(r == 0, 1, 0), 0)
        return here & fresh, here & (8 * q + r > 0), remote(
            b_all.at[2, q], b_all.at[3, down_slot], b_send.at[1, q], b_recv.at[3, down_slot], at_row(rem(r + 7, 8))
        ), remote(b_all.at[2, q], b_all.at[2, q], b_send.at[2, q], b_recv.at[2, q], place(k=1 - k))

    def column_role(f):
        i0 = c - f + 1
        exists = (i0 >= 0) & (i0 < N_COL)
        r0 = rem(i0 + 8, 8)
        dx = rem(x - rem(r0, 4) + 4, 4)
        same = zl == div(r0, 4)
        return exists, dx, same

    def column_copies(f, t):
        exists, dx, same = column_role(f)
        half = x_col.at[f, pl.ds(t * HALF, HALF), :]

        def to(n, where):
            return remote(half, half, col_send.at[t, n], col_recv.at[f, t], where)

        source = exists & (dx == 0) & same
        for n in range(7):
            there_zl = zl if n < 3 else 1 - zl
            there_x = rem(x + (3, 1, 2, 0, 3, 1, 2)[n], 4)
            apart = rem(r - there_zl * 4 - there_x + 8, 8)
            chained = (apart <= FRONTS - 1 - f) & (c - f + 1 - apart >= 0)
            yield source & jnp.logical_not(chained), to(n, place(zl=there_zl, x=there_x))

    def column_arrival(f, t):
        exists, dx, same = column_role(f)
        half = x_col.at[f, pl.ds(t * HALF, HALF), :]
        source = (dx == 0) & same
        return exists & jnp.logical_not(source | (owner & (own_front > f))), remote(
            half, half, col_send.at[t, 0], col_recv.at[f, t], place(zl=1 - zl)
        )

    def row_role(f, q):
        total = r + f + 7
        place_in = rem(total, 8)
        plane = q + div(total, 8) - 1
        dy = rem(y - div(place_in, 2) + 4, 4)
        same = k == rem(place_in, 2)
        return plane, (plane >= 0) & (plane <= zh), dy, same

    def row_copies(f, q, t):
        plane, present, dy, same = row_role(f, q)
        half = x_row.at[f, q, pl.ds(t * HALF, HALF), :]

        def to(sem, where):
            return remote(half, half, sem, row_recv.at[f, q, t], where)

        carrier = present & same
        yield carrier, to(row_send.at[div(f, 2), q, t, 0], place(k=1 - k))
        if t == 0:
            direct = f < 2
            yield carrier & ((dy == 0) | (dy == 2) | ((dy == 1) & jnp.logical_not(direct))), to(
                row_send.at[div(f, 2), q, t, 1], place(y=rem(y + 1, 4))
            )
            yield carrier & (dy == 0) & direct, to(row_send.at[div(f, 2), q, t, 2], place(y=rem(y + 2, 4)))
        else:
            yield carrier & (dy != 1), to(row_send.at[div(f, 2), q, t, 1], place(y=rem(y + 3, 4)))

    def far_copies(f, q, t):
        half = x_row.at[f, q, pl.ds(t * HALF, HALF), :]
        for by in (1, 2, 3):
            yield zh + by < 4, remote(
                half, half, row_far.at[t, by - 1], row_recv.at[f, q, t], place(zh=jnp.minimum(zh + by, 3))
            )

    def row_arrival(f, q, t):
        plane, present, dy, same = row_role(f, q)
        half = x_row.at[f, q, pl.ds(t * HALF, HALF), :]
        source = (plane == zh) & (dy == 0) & same
        return present & jnp.logical_not(source), remote(
            half, half, row_send.at[div(f, 2), q, t, 0], row_recv.at[f, q, t], place(k=1 - k)
        )

    def start(condition, copy):
        @pl.when(condition)
        def _():
            copy.start()

    def drain(condition, copy):
        @pl.when(condition)
        def _():
            copy.wait_send()

    def land(condition, copy):
        @pl.when(condition)
        def _():
            copy.wait_recv()

    def land_a(f, q, wanted):
        land(wanted, remote(a_all.at[f, q], a_all.at[f, q], a_send.at[f, q], a_recv.at[f, q], place(k=1 - k)))

    def land_b(f, q, wanted):
        land(wanted, remote(b_all.at[f, q], b_all.at[f, q], b_send.at[f, q], b_recv.at[f, q], place(k=1 - k)))

    def subtract_upper(f, q, solved):
        put_work(q, block_of(work, q) - matmul(block_of(a_all, f, q), solved))

    def subtract_lower(f, q, solved):
        put_work(q, block_of(work, q) - matmul(solved, block_of(b_all, f, q)))

    def update(f, q):
        ahead = c - 8 * q - r
        open_block = jnp.logical_not(owner & (q == own_slot))
        upper = c - f + 1 < N_COL
        lower = 8 * q + r + f - 1 >= 0
        both = open_block & (ahead >= f + 1) & upper & lower
        for g, pending in ((f, open_block & (ahead >= f)), (f + 1, open_block & (ahead >= f + 1))):
            land_a(g, q, pending & (c - g + 1 < N_COL) & ((g == 0) | (g == 3)))
            land_b(
                g, q, pending & (8 * q + r + g - 1 >= 0) & ((g == 0) | (g == 3) | ((g == 2) & jnp.logical_not(hands_on)))
            )

        @pl.when(both)
        def _():
            left = jnp.concatenate(
                [block_of(a_all, f, q), block_of(a_all, f + 1, q), x_row[f, q], x_row[f + 1, q]], axis=1
            )
            right = jnp.concatenate(
                [x_col[f], x_col[f + 1], block_of(b_all, f, q), block_of(b_all, f + 1, q)], axis=0
            )
            put_work(q, block_of(work, q) - matmul(left, right))

        def one(g, carry):
            pending = open_block & jnp.logical_not(both) & (ahead >= g)

            @pl.when(pending & (c - g + 1 < N_COL))
            def _():
                subtract_upper(g, q, x_col[g])

            @pl.when(pending & (8 * q + r + g - 1 >= 0))
            def _():
                subtract_lower(g, q, x_row[g, q])

            return carry

        lax.fori_loop(f, f + 2, one, 0)

    def chain_copies(f, row, column):
        wanted = owner & (own_front < FRONTS - 1)
        yield wanted & (c + 1 < N_COL), remote(
            row, chain_row.at[f], chain_send.at[0, f], chain_recv.at[0, f], at_column(jnp.minimum(c + 1, N_COL - 1))
        )
        yield wanted & (8 * own_slot + r > 0), remote(
            column, x_col.at[f], chain_send.at[1, f], chain_recv.at[1, f], at_row(rem(r + 7, 8))
        )

    def relayed(f):
        return chain_copies(f, chain_row.at[f], x_col.at[f])

    def own_copies():
        f = jnp.minimum(own_front, FRONTS - 2)
        return chain_copies(f, x_row.at[f, slot], x_col.at[f])

    def send_shifts(wanted):
        def one(step, carry):
            for first, condition, copy in shift_copies(N_SLOT - 1 - step):
                if first == wanted:
                    start(condition, copy)
            return carry

        lax.fori_loop(0, N_SLOT, one, 0)

    mine = rem(k + r + 1, 2)

    def receive_row(f, q, t, wanted):
        arriving, arrival = row_arrival(f, q, t)

        @pl.when(arriving & wanted)
        def _():
            with jax.named_scope(f"row#t={t}"):
                arrival.wait_recv()
            for condition, copy in row_copies(f, q, t):
                start(condition, copy)

    deferred = owner & (own_front < FRONTS - 2)
    even_row = rem(r, 2) == 0
    after_arrival = owner & ((distance == 1) | (distance == 2) | ((distance == 0) & even_row))
    fourth = (distance == 4) & (k == 1)
    beside = ((k == 0) & ((distance == 6) | (distance == 7) | ((distance == 0) & (x != 0)))) | fourth
    beside_front = jnp.where(beside & jnp.logical_not(fourth), rem(distance + 2, 8), 0)
    nearest = zh - div(r + beside_front + 7, 8) + 1
    watches = beside & (nearest >= 0) & (nearest < N_SLOT)
    watched = jnp.clip(nearest, 0, N_SLOT - 1)

    def watch():
        for t in (0, 1):
            receive_row(beside_front, watched, t, True)

    solves_later = (distance == 7) | (distance == 0)
    send_shifts(0)

    @pl.when(jnp.logical_not(after_arrival | fourth))
    def _():
        send_shifts(4)

    @pl.when(watches & jnp.logical_not(solves_later))
    def _():
        watch()

    @pl.when(fourth)
    def _():
        send_shifts(4)

    middle = (distance >= 3) & (distance <= 5)

    @pl.when(jnp.logical_not(deferred))
    def _():
        send_shifts(1)

    @pl.when(middle)
    def _():
        send_shifts(3)

    @pl.when(owner)
    def _():
        row_first = ((k == 1) | (rem(r, 4) == 3)) & (rem(c, 8) != 0)

        def earlier(step, carry):
            f = div(step, 2)
            take_row = (rem(step, 2) == 0) == row_first

            @pl.when((f < own_front) & jnp.logical_not(take_row) & (c - f + 1 < N_COL))
            def _():
                with jax.named_scope("chain_col"):
                    land(True, remote(x_col.at[f], x_col.at[f], chain_send.at[1, 0], chain_recv.at[1, f], place(k=1 - k)))
                start(*list(relayed(f))[1])
                with jax.named_scope("chain_upper"):
                    land_a(f, slot, f != 1)
                    subtract_upper(f, slot, x_col[f])

            @pl.when((f < own_front) & take_row & (8 * slot + r + f - 1 >= 0))
            def _():
                with jax.named_scope("chain_row"):
                    land(True, remote(chain_row.at[f], chain_row.at[f], chain_send.at[0, 0], chain_recv.at[0, f], place(k=1 - k)))
                start(*list(relayed(f))[0])
                with jax.named_scope("chain_lower"):
                    land_b(f, slot, f != 1)
                    subtract_lower(f, slot, chain_row[f])

            @pl.when(after_arrival & (step == 0))
            def _():
                send_shifts(4)

            return carry

        lax.fori_loop(0, 2 * (FRONTS - 1), earlier, 0)
        with jax.named_scope("solve"):
            rotated = matmul(matmul(ia[...], block_of(work, slot)), vb[...])
            solved = matmul(matmul(va[...], rotated / denominator[...]), ib[...])
            x_col[own_front] = solved
            x_row[own_front, slot] = solved
            put_work(slot, solved)
        for condition, copy in own_copies():
            start(condition, copy)
        for t in (0, 1):
            for condition, copy in far_copies(own_front, slot, t):
                start(condition, copy)
        for t in (0, 1):
            for condition, copy in column_copies(own_front, t):
                start(condition, copy)
            for condition, copy in row_copies(own_front, slot, t):
                start(condition, copy)

    @pl.when(watches & solves_later)
    def _():
        watch()

    @pl.when(deferred)
    def _():
        send_shifts(1)

    crosses_soon = owner | ((r == 0) & (distance == 6))

    @pl.when(crosses_soon)
    def _():
        send_shifts(2)

    @pl.when(jnp.logical_not(middle))
    def _():
        send_shifts(3)

    def receive_column(f):
        for t in (0, 1):
            with jax.named_scope(f"col#t={t}"):
                land(*column_arrival(f, t))

    def pass_on(which):
        def one(step, carry):
            arrived, forwarded, copy, arrival = which(N_SLOT - 1 - step)
            land(arrived, arrival)
            start(forwarded, copy)
            return carry

        with jax.named_scope("pass"):
            lax.fori_loop(0, N_SLOT, one, 0)

    soon = (x >= 2) & (distance >= 3) & (distance <= 6)

    def ring(f, opening):
        def one(step, carry):
            n = div(step, N_SLOT)
            q = N_SLOT - 1 - rem(step, N_SLOT)
            _, _, dy, _ = row_role(f, q)
            receive_row(f, q, 0, dy == n)
            receive_row(f, q, 1, rem(4 - dy, 4) == n)

            @pl.when(soon & opening & (step == 2 * N_SLOT - 1))
            def _():
                pass_on(handed_copy)

            return carry

        lax.fori_loop(0, 4 * N_SLOT, one, 0)

    late = (distance == 1) | (distance == 2)
    ring(jnp.where(late, mine + 2, mine), True)

    @pl.when(jnp.logical_not(crosses_soon))
    def _():
        send_shifts(2)

    @pl.when(jnp.logical_not(soon))
    def _():
        pass_on(handed_copy)

    def pair(f):
        for g in (f, f + 1):
            receive_column(g)

        def one(step, carry):
            q = N_SLOT - 1 - step
            for g in (f, f + 1):
                leaf = (rem(g, 2) != mine) & jnp.logical_not(watches & (g == beside_front) & (q == nearest))
                for t in (0, 1):
                    receive_row(g, q, t, leaf)
            with jax.named_scope("bulk"):
                update(f, q)
            return carry

        lax.fori_loop(0, N_SLOT, one, 0)

    early = (mine == 1) & ((distance == 0) | (distance >= 4)) & (x != 0) & (rem(c, 8) != 7)

    def stage(j, carry):
        @pl.when(j == 1)
        def _():
            ring(jnp.where(late, mine, mine + 2), False)
            pass_on(passed_copy)

        @pl.when((j == 3) | ((j == 0) & early) | ((j == 2) & jnp.logical_not(early)))
        def _():
            pair(jnp.where(j == 3, 2, 0))

        return carry

    lax.fori_loop(0, 4, stage, 0)

    def finish(q, carry):
        for _, condition, copy in shift_copies(q):
            drain(condition, copy)
        for _, forwarded, copy, _ in (passed_copy(q), handed_copy(q)):
            drain(forwarded, copy)
        return carry

    with jax.named_scope("finish"):
        lax.fori_loop(0, N_SLOT, finish, 0)

    def finish_front(f, carry):
        for t in (0, 1):
            for condition, copy in column_copies(f, t):
                drain(condition, copy)

        def one(q, carry):
            for t in (0, 1):
                for condition, copy in row_copies(f, q, t):
                    drain(condition, copy)
            return carry

        return lax.fori_loop(0, N_SLOT, one, carry)

    with jax.named_scope("finish_front"):
        lax.fori_loop(0, FRONTS, finish_front, 0)

    @pl.when(owner)
    def _():
        for condition, copy in own_copies():
            drain(condition, copy)

        def finish_chain(f, carry):
            beside, above = relayed(f)
            drain((f < own_front) & (8 * slot + r + f - 1 >= 0) & beside[0], beside[1])
            drain((f < own_front) & (c - f + 1 < N_COL) & above[0], above[1])
            return carry

        lax.fori_loop(0, FRONTS - 1, finish_chain, 0)
        for t in (0, 1):
            for condition, copy in far_copies(own_front, slot, t):
                drain(condition, copy)


def body(
    upper_a, upper_b, right_side, vectors_a, inverse_a, values_a, vectors_b, inverse_b, values_b
):
    tall = (N_SLOT, 2 * BLOCK, HALF)
    square = (N_SLOT, BLOCK, BLOCK)
    anywhere = pl.BlockSpec(memory_space=pl.ANY)
    inside = pl.BlockSpec(memory_space=pltpu.VMEM)
    dma = pltpu.SemaphoreType.DMA
    solved = pl.pallas_call(
        kernel,
        out_shape=pltpu.VMEM(tall, jnp.float32),
        in_specs=[anywhere] * 5 + [inside] + [anywhere] * 2 + [inside],
        out_specs=inside,
        scratch_shapes=[
            pltpu.VMEM((FRONTS, *tall), jnp.float32),
            pltpu.VMEM((FRONTS, *tall), jnp.float32),
            pltpu.VMEM(square, jnp.float32),
            pltpu.VMEM((FRONTS, *square), jnp.float32),
            pltpu.VMEM((FRONTS - 1, BLOCK, BLOCK), jnp.float32),
            *[pltpu.VMEM((BLOCK, BLOCK), jnp.float32)] * 5,
            dma((4, N_SLOT)),
            dma((4, N_SLOT)),
            dma((4, N_SLOT)),
            dma((4, N_SLOT)),
            dma((FRONTS // 2, N_SLOT, 2, 3)),
            dma((2, 3)),
            dma((FRONTS, N_SLOT, 2)),
            dma((2, 7)),
            dma((FRONTS, 2)),
            dma((2, 3)),
            dma((2, 3)),
            dma((7,)),
        ],
        compiler_params=pltpu.CompilerParams(
            collective_id=0, has_side_effects=True, vmem_limit_bytes=60 * 1024 * 1024
        ),
    )(
        upper_a.reshape(tall), upper_b.reshape(tall), right_side.reshape(tall),
        vectors_a.reshape(square), inverse_a.reshape(square), values_a.reshape(2 * N_SLOT, HALF),
        vectors_b.reshape(BLOCK, BLOCK), inverse_b.reshape(BLOCK, BLOCK), values_b.reshape(2, HALF),
    )
    return solved.reshape(right_side.shape)


def solution(mesh):
    finer = Mesh(mesh.devices.reshape(2, 4, 4, 4, 2), ROW + COL)
    whole = P(None, ROW, None, COL, None)
    placed = (
        whole, whole, whole,
        P(None, ROW, None, None), P(None, ROW, None, None), P(None, ROW, None),
        P(COL, None, None), P(COL, None, None), P(COL, None),
    )
    return jax.shard_map(body, mesh=finer, in_specs=placed, out_specs=whole, check_vma=False)
```

```python
import functools

import jax
import jax.numpy as jnp
from jax import lax
from jax.experimental import pallas as pl
from jax.experimental.pallas import tpu as pltpu
from jax.sharding import Mesh
from jax.sharding import PartitionSpec as P

FRONTS = 4
N_SLOT = 4
BLOCK = 256
HALF = 128
N_COL = 32
MESH = pl.DeviceIdType.MESH
ROW = ("zl", "x")
COL = ("zh", "y", "k")


def parts(value):
    high = value.astype(jnp.bfloat16)
    low = (value - high.astype(jnp.float32)).astype(jnp.bfloat16)
    return high, low


def matmul(former, latter):
    former_high, former_low = parts(former)
    latter_high, latter_low = parts(latter)
    left = jnp.concatenate([former_high, former_low, former_high], axis=1)
    right = jnp.concatenate([latter_high, latter_high, latter_low], axis=0)
    return jnp.dot(left, right, preferred_element_type=jnp.float32)


def kernel(
    a_hbm, b_hbm, w_hbm, va_hbm, ia_hbm, la_ref, vb_hbm, ib_hbm, lb_ref, work,
    a_all, b_all, x_col, x_row, chain_row, va, ia, vb, ib, denominator,
    a_send, a_recv, b_send, b_recv, row_send, row_far, row_recv, col_send, col_recv, chain_send, chain_recv, local,
):
    zl, x = lax.axis_index("zl"), lax.axis_index("x")
    zh, y, k = lax.axis_index("zh"), lax.axis_index("y"), lax.axis_index("k")
    r = zl * 4 + x
    c = zh * 8 + y * 2 + k
    rem, div = lax.rem, lax.div

    def place(zl=zl, x=x, zh=zh, y=y, k=k):
        return {"zl": zl, "x": x, "zh": zh, "y": y, "k": k}

    def at_column(j):
        return place(zh=div(j, 8), y=div(rem(j, 8), 2), k=rem(j, 2))

    def at_row(i):
        return place(zl=div(i, 4), x=rem(i, 4))

    def remote(src, dst, send_sem, recv_sem, where):
        return pltpu.make_async_remote_copy(
            src_ref=src, dst_ref=dst, send_sem=send_sem, recv_sem=recv_sem,
            device_id=where, device_id_type=MESH,
        )

    own_front = rem(c - r + 33, 8)
    own_slot = div(c - r - own_front + 1 + 64, 8) - 8
    owner = (own_front < FRONTS) & (own_slot >= 0) & (own_slot < N_SLOT)
    slot = jnp.clip(own_slot, 0, N_SLOT - 1)

    loads = [
        pltpu.make_async_copy(w_hbm, work, local.at[0]),
        pltpu.make_async_copy(a_hbm, a_all.at[1], local.at[1]),
        pltpu.make_async_copy(b_hbm, b_all.at[1], local.at[2]),
    ]
    factor_loads = [
        pltpu.make_async_copy(ia_hbm.at[slot], ia, local.at[3]),
        pltpu.make_async_copy(vb_hbm, vb, local.at[4]),
        pltpu.make_async_copy(va_hbm.at[slot], va, local.at[5]),
        pltpu.make_async_copy(ib_hbm, ib, local.at[6]),
    ]
    loads[0].start()

    @pl.when(owner)
    def _():
        for load in factor_loads:
            load.start()

    loads[1].start()
    loads[2].start()

    barrier = pltpu.get_barrier_semaphore()
    friends = [at_column(rem(c + by, N_COL)) for by in (1, 31, 2, 30)]
    friends += [at_row(rem(r + by, 8)) for by in range(1, 8)]
    friends += [place(k=1 - k)] + [place(y=rem(y + by, 4)) for by in (1, 2, 3)]
    friends += [place(zh=rem(zh + by, 4)) for by in (1, 2, 3)]
    for friend in friends:
        pl.semaphore_signal(barrier, inc=1, device_id=friend, device_id_type=MESH)

    @pl.when(owner)
    def _():
        left = jnp.concatenate(
            [la_ref[pl.ds(2 * slot, 1), :], la_ref[pl.ds(2 * slot + 1, 1), :]], axis=1
        )
        right = jnp.concatenate([lb_ref[pl.ds(0, 1), :], lb_ref[pl.ds(1, 1), :]], axis=1)
        denominator[...] = jnp.broadcast_to(left, (BLOCK, BLOCK)).T + right
        for load in factor_loads:
            load.wait()

    with jax.named_scope("barrier"):
        pl.semaphore_wait(barrier, len(friends))
    with jax.named_scope("loads"):
        for load in loads:
            load.wait()

    def block_of(ref, *index):
        return jnp.concatenate(
            [ref[(*index, pl.ds(0, BLOCK, 2), slice(None))], ref[(*index, pl.ds(1, BLOCK, 2), slice(None))]],
            axis=1,
        )

    def put_work(q, value):
        work[q, pl.ds(0, BLOCK, 2), :] = value[:, :HALF]
        work[q, pl.ds(1, BLOCK, 2), :] = value[:, HALF:]

    distance = rem(c - r + 32, 8)
    near_slot = div(c - 1 - r + 8, 8) - 1

    def shift_copies(q):
        above = 8 * q + r < c
        near = (q == near_slot) & (distance >= 1) & (distance <= 3)
        nearer = near & (distance == 1)
        crossing = (rem(c, 8) >= 6) & (x != 1) & ((x == 0) | (zl == 1))
        first_row = jnp.where(r == 0, 1, 0)
        second_row = jnp.where(r <= 1, 1, 0)
        left = at_column(jnp.maximum(c - 1, 0))
        right = at_column(jnp.minimum(c + 1, N_COL - 1))
        farther = at_column(jnp.minimum(c + 2, N_COL - 1))
        below, higher, highest = at_row(rem(r + 1, 8)), at_row(rem(r + 7, 8)), at_row(rem(r + 6, 8))

        def a_copy(f, where):
            return remote(a_hbm.at[q], a_all.at[f, q], a_send.at[f, q], a_recv.at[f, q], where)

        def b_copy(f, there, where):
            target = jnp.clip(there, 0, N_SLOT - 1)
            return remote(b_hbm.at[q], b_all.at[f, target], b_send.at[f, q], b_recv.at[f, target], where)

        sends = [
            (above, near, None, a_copy(0, left)),
            (above, near, None, b_copy(0, q + div(r, 7), below)),
            (above & (c + 1 < N_COL), nearer, crossing & (k == 1), a_copy(2, right)),
            (above & (8 * q + r >= 1), nearer, None, b_copy(2, q - first_row, higher)),
        ]
        for number, (wanted, soon, later, copy) in enumerate(sends):
            yield 0, wanted & soon, copy
            rest = wanted & jnp.logical_not(soon)
            if later is None:
                yield 4 if number < 2 else 1, rest, copy
            else:
                yield 1, rest & jnp.logical_not(later), copy
                yield 2, rest & later, copy
        wanted = above & (c + 2 < N_COL) & (k == 0)
        yield 1, wanted & jnp.logical_not(crossing), a_copy(3, farther)
        yield 2, wanted & crossing, a_copy(3, farther)
        yield 3, above & (x == 2), b_copy(3, q - second_row, highest)

    def passed_copy(q):
        fresh = jnp.logical_not(owner & (own_front == 3) & (q == own_slot))
        here = 8 * q + r < c - 1
        return here & fresh, here & (k == 0), remote(
            a_all.at[2, q], a_all.at[3, q], a_send.at[1, q], a_recv.at[3, q], place(k=1 - k)
        ), remote(a_all.at[2, q], a_all.at[2, q], a_send.at[2, q], a_recv.at[2, q], place(k=1 - k))

    hands_on = x != 1

    def handed_copy(q):
        fresh = jnp.logical_not(owner & (own_front == 3) & (q == own_slot))
        here = hands_on & (8 * q + r + 1 < c)
        down_slot = jnp.maximum(q - jnp.where(r == 0, 1, 0), 0)
        return here & fresh, here & (8 * q + r > 0), remote(
            b_all.at[2, q], b_all.at[3, down_slot], b_send.at[1, q], b_recv.at[3, down_slot], at_row(rem(r + 7, 8))
        ), remote(b_all.at[2, q], b_all.at[2, q], b_send.at[2, q], b_recv.at[2, q], place(k=1 - k))

    def column_role(f):
        i0 = c - f + 1
        exists = (i0 >= 0) & (i0 < N_COL)
        r0 = rem(i0 + 8, 8)
        dx = rem(x - rem(r0, 4) + 4, 4)
        same = zl == div(r0, 4)
        return exists, dx, same

    def column_copies(f, t):
        exists, dx, same = column_role(f)
        half = x_col.at[f, pl.ds(t * HALF, HALF), :]

        def to(n, where):
            return remote(half, half, col_send.at[t, n], col_recv.at[f, t], where)

        source = exists & (dx == 0) & same
        for n in range(7):
            there_zl = zl if n < 3 else 1 - zl
            there_x = rem(x + (3, 1, 2, 0, 3, 1, 2)[n], 4)
            apart = rem(r - there_zl * 4 - there_x + 8, 8)
            chained = (apart <= FRONTS - 1 - f) & (c - f + 1 - apart >= 0)
            yield source & jnp.logical_not(chained), to(n, place(zl=there_zl, x=there_x))

    def column_arrival(f, t):
        exists, dx, same = column_role(f)
        half = x_col.at[f, pl.ds(t * HALF, HALF), :]
        source = (dx == 0) & same
        return exists & jnp.logical_not(source | (owner & (own_front > f))), remote(
            half, half, col_send.at[t, 0], col_recv.at[f, t], place(zl=1 - zl)
        )

    def row_role(f, q):
        total = r + f + 7
        place_in = rem(total, 8)
        plane = q + div(total, 8) - 1
        dy = rem(y - div(place_in, 2) + 4, 4)
        same = k == rem(place_in, 2)
        return plane, (plane >= 0) & (plane <= zh), dy, same

    def row_copies(f, q, t):
        plane, present, dy, same = row_role(f, q)
        half = x_row.at[f, q, pl.ds(t * HALF, HALF), :]

        def to(sem, where):
            return remote(half, half, sem, row_recv.at[f, q, t], where)

        carrier = present & same
        yield carrier, to(row_send.at[div(f, 2), q, t, 0], place(k=1 - k))
        if t == 0:
            direct = f < 2
            yield carrier & ((dy == 0) | (dy == 2) | ((dy == 1) & jnp.logical_not(direct))), to(
                row_send.at[div(f, 2), q, t, 1], place(y=rem(y + 1, 4))
            )
            yield carrier & (dy == 0) & direct, to(row_send.at[div(f, 2), q, t, 2], place(y=rem(y + 2, 4)))
        else:
            yield carrier & (dy != 1), to(row_send.at[div(f, 2), q, t, 1], place(y=rem(y + 3, 4)))

    def far_copies(f, q, t):
        half = x_row.at[f, q, pl.ds(t * HALF, HALF), :]
        for by in (1, 2, 3):
            yield zh + by < 4, remote(
                half, half, row_far.at[t, by - 1], row_recv.at[f, q, t], place(zh=jnp.minimum(zh + by, 3))
            )

    def row_arrival(f, q, t):
        plane, present, dy, same = row_role(f, q)
        half = x_row.at[f, q, pl.ds(t * HALF, HALF), :]
        source = (plane == zh) & (dy == 0) & same
        return present & jnp.logical_not(source), remote(
            half, half, row_send.at[div(f, 2), q, t, 0], row_recv.at[f, q, t], place(k=1 - k)
        )

    def start(condition, copy):
        @pl.when(condition)
        def _():
            copy.start()

    def drain(condition, copy):
        @pl.when(condition)
        def _():
            copy.wait_send()

    def land(condition, copy):
        @pl.when(condition)
        def _():
            copy.wait_recv()

    def land_a(f, q, wanted):
        land(wanted, remote(a_all.at[f, q], a_all.at[f, q], a_send.at[f, q], a_recv.at[f, q], place(k=1 - k)))

    def land_b(f, q, wanted):
        land(wanted, remote(b_all.at[f, q], b_all.at[f, q], b_send.at[f, q], b_recv.at[f, q], place(k=1 - k)))

    def subtract_upper(f, q, solved):
        put_work(q, block_of(work, q) - matmul(block_of(a_all, f, q), solved))

    def subtract_lower(f, q, solved):
        put_work(q, block_of(work, q) - matmul(solved, block_of(b_all, f, q)))

    def update(f, q):
        ahead = c - 8 * q - r
        open_block = jnp.logical_not(owner & (q == own_slot))
        upper = c - f + 1 < N_COL
        lower = 8 * q + r + f - 1 >= 0
        both = open_block & (ahead >= f + 1) & upper & lower
        for g, pending in ((f, open_block & (ahead >= f)), (f + 1, open_block & (ahead >= f + 1))):
            land_a(g, q, pending & (c - g + 1 < N_COL) & ((g == 0) | (g == 3)))
            land_b(
                g, q, pending & (8 * q + r + g - 1 >= 0) & ((g == 0) | (g == 3) | ((g == 2) & jnp.logical_not(hands_on)))
            )

        @pl.when(both)
        def _():
            left = jnp.concatenate(
                [block_of(a_all, f, q), block_of(a_all, f + 1, q), x_row[f, q], x_row[f + 1, q]], axis=1
            )
            right = jnp.concatenate(
                [x_col[f], x_col[f + 1], block_of(b_all, f, q), block_of(b_all, f + 1, q)], axis=0
            )
            put_work(q, block_of(work, q) - matmul(left, right))

        def one(g, carry):
            pending = open_block & jnp.logical_not(both) & (ahead >= g)

            @pl.when(pending & (c - g + 1 < N_COL))
            def _():
                subtract_upper(g, q, x_col[g])

            @pl.when(pending & (8 * q + r + g - 1 >= 0))
            def _():
                subtract_lower(g, q, x_row[g, q])

            return carry

        lax.fori_loop(f, f + 2, one, 0)

    def chain_copies(f, row, column):
        wanted = owner & (own_front < FRONTS - 1)
        yield wanted & (c + 1 < N_COL), remote(
            row, chain_row.at[f], chain_send.at[0, f], chain_recv.at[0, f], at_column(jnp.minimum(c + 1, N_COL - 1))
        )
        yield wanted & (8 * own_slot + r > 0), remote(
            column, x_col.at[f], chain_send.at[1, f], chain_recv.at[1, f], at_row(rem(r + 7, 8))
        )

    def relayed(f):
        return chain_copies(f, chain_row.at[f], x_col.at[f])

    def own_copies():
        f = jnp.minimum(own_front, FRONTS - 2)
        return chain_copies(f, x_row.at[f, slot], x_col.at[f])

    def send_shifts(wanted):
        def one(step, carry):
            for first, condition, copy in shift_copies(N_SLOT - 1 - step):
                if first == wanted:
                    start(condition, copy)
            return carry

        lax.fori_loop(0, N_SLOT, one, 0)

    mine = rem(k + r + 1, 2)

    def receive_row(f, q, t, wanted):
        arriving, arrival = row_arrival(f, q, t)

        @pl.when(arriving & wanted)
        def _():
            with jax.named_scope(f"row#t={t}"):
                arrival.wait_recv()
            for condition, copy in row_copies(f, q, t):
                start(condition, copy)

    deferred = owner & (own_front < FRONTS - 2)
    even_row = rem(r, 2) == 0
    after_arrival = owner & ((distance == 1) | (distance == 2) | ((distance == 0) & even_row))
    fourth = (distance == 4) & (k == 1)
    beside = ((k == 0) & ((distance == 6) | (distance == 7) | ((distance == 0) & (x != 0)))) | fourth
    beside_front = jnp.where(beside & jnp.logical_not(fourth), rem(distance + 2, 8), 0)
    nearest = zh - div(r + beside_front + 7, 8) + 1
    watches = beside & (nearest >= 0) & (nearest < N_SLOT)
    watched = jnp.clip(nearest, 0, N_SLOT - 1)

    def watch():
        for t in (0, 1):
            receive_row(beside_front, watched, t, True)

    solves_later = (distance == 7) | (distance == 0)
    send_shifts(0)

    @pl.when(jnp.logical_not(after_arrival | fourth))
    def _():
        send_shifts(4)

    @pl.when(watches & jnp.logical_not(solves_later))
    def _():
        watch()

    @pl.when(fourth)
    def _():
        send_shifts(4)

    middle = (distance >= 3) & (distance <= 5)

    @pl.when(jnp.logical_not(deferred))
    def _():
        send_shifts(1)

    @pl.when(middle)
    def _():
        send_shifts(3)

    @pl.when(owner)
    def _():
        row_first = ((k == 1) | (rem(r, 4) == 3)) & (rem(c, 8) != 0)

        def earlier(step, carry):
            f = div(step, 2)
            take_row = (rem(step, 2) == 0) == row_first

            @pl.when((f < own_front) & jnp.logical_not(take_row) & (c - f + 1 < N_COL))
            def _():
                with jax.named_scope("chain_col"):
                    land(True, remote(x_col.at[f], x_col.at[f], chain_send.at[1, 0], chain_recv.at[1, f], place(k=1 - k)))
                start(*list(relayed(f))[1])
                with jax.named_scope("chain_upper"):
                    land_a(f, slot, f != 1)
                    subtract_upper(f, slot, x_col[f])

            @pl.when((f < own_front) & take_row & (8 * slot + r + f - 1 >= 0))
            def _():
                with jax.named_scope("chain_row"):
                    land(True, remote(chain_row.at[f], chain_row.at[f], chain_send.at[0, 0], chain_recv.at[0, f], place(k=1 - k)))
                start(*list(relayed(f))[0])
                with jax.named_scope("chain_lower"):
                    land_b(f, slot, f != 1)
                    subtract_lower(f, slot, chain_row[f])

            @pl.when(after_arrival & (step == 0))
            def _():
                send_shifts(4)

            return carry

        lax.fori_loop(0, 2 * (FRONTS - 1), earlier, 0)
        with jax.named_scope("solve"):
            rotated = matmul(matmul(ia[...], block_of(work, slot)), vb[...])
            solved = matmul(matmul(va[...], rotated / denominator[...]), ib[...])
            x_col[own_front] = solved
            x_row[own_front, slot] = solved
            put_work(slot, solved)
        for condition, copy in own_copies():
            start(condition, copy)
        for t in (0, 1):
            for condition, copy in far_copies(own_front, slot, t):
                start(condition, copy)
        for t in (0, 1):
            for condition, copy in column_copies(own_front, t):
                start(condition, copy)
            for condition, copy in row_copies(own_front, slot, t):
                start(condition, copy)

    @pl.when(watches & solves_later)
    def _():
        watch()

    @pl.when(deferred)
    def _():
        send_shifts(1)

    crosses_soon = owner | ((r == 0) & (distance == 6)) | ((r == 2) | (r == 3))

    @pl.when(crosses_soon)
    def _():
        send_shifts(2)

    @pl.when(jnp.logical_not(middle))
    def _():
        send_shifts(3)

    def receive_column(f):
        for t in (0, 1):
            with jax.named_scope(f"col#t={t}"):
                land(*column_arrival(f, t))

    def pass_on(which):
        def one(step, carry):
            arrived, forwarded, copy, arrival = which(N_SLOT - 1 - step)
            land(arrived, arrival)
            start(forwarded, copy)
            return carry

        with jax.named_scope("pass"):
            lax.fori_loop(0, N_SLOT, one, 0)

    soon = (x >= 2) & (distance >= 3) & (distance <= 6)

    def ring(f, opening):
        def one(step, carry):
            n = div(step, N_SLOT)
            q = N_SLOT - 1 - rem(step, N_SLOT)
            _, _, dy, _ = row_role(f, q)
            receive_row(f, q, 0, dy == n)
            receive_row(f, q, 1, rem(4 - dy, 4) == n)

            @pl.when(soon & opening & (step == 2 * N_SLOT - 1))
            def _():
                pass_on(handed_copy)

            return carry

        lax.fori_loop(0, 4 * N_SLOT, one, 0)

    late = (distance == 1) | (distance == 2)
    ring(jnp.where(late, mine + 2, mine), True)

    @pl.when(jnp.logical_not(crosses_soon))
    def _():
        send_shifts(2)

    @pl.when(jnp.logical_not(soon))
    def _():
        pass_on(handed_copy)

    def pair(f):
        for g in (f, f + 1):
            receive_column(g)

        def one(step, carry):
            q = N_SLOT - 1 - step
            for g in (f, f + 1):
                leaf = (rem(g, 2) != mine) & jnp.logical_not(watches & (g == beside_front) & (q == nearest))
                for t in (0, 1):
                    receive_row(g, q, t, leaf)
            with jax.named_scope("bulk"):
                update(f, q)
            return carry

        lax.fori_loop(0, N_SLOT, one, 0)

    early = (mine == 1) & ((distance == 0) | (distance >= 4)) & (x != 0) & (rem(c, 8) != 7)

    def stage(j, carry):
        @pl.when(j == 1)
        def _():
            ring(jnp.where(late, mine, mine + 2), False)
            pass_on(passed_copy)

        @pl.when((j == 3) | ((j == 0) & early) | ((j == 2) & jnp.logical_not(early)))
        def _():
            pair(jnp.where(j == 3, 2, 0))

        return carry

    lax.fori_loop(0, 4, stage, 0)

    def finish(q, carry):
        for _, condition, copy in shift_copies(q):
            drain(condition, copy)
        for _, forwarded, copy, _ in (passed_copy(q), handed_copy(q)):
            drain(forwarded, copy)
        return carry

    with jax.named_scope("finish"):
        lax.fori_loop(0, N_SLOT, finish, 0)

    def finish_front(f, carry):
        for t in (0, 1):
            for condition, copy in column_copies(f, t):
                drain(condition, copy)

        def one(q, carry):
            for t in (0, 1):
                for condition, copy in row_copies(f, q, t):
                    drain(condition, copy)
            return carry

        return lax.fori_loop(0, N_SLOT, one, carry)

    with jax.named_scope("finish_front"):
        lax.fori_loop(0, FRONTS, finish_front, 0)

    @pl.when(owner)
    def _():
        for condition, copy in own_copies():
            drain(condition, copy)

        def finish_chain(f, carry):
            beside, above = relayed(f)
            drain((f < own_front) & (8 * slot + r + f - 1 >= 0) & beside[0], beside[1])
            drain((f < own_front) & (c - f + 1 < N_COL) & above[0], above[1])
            return carry

        lax.fori_loop(0, FRONTS - 1, finish_chain, 0)
        for t in (0, 1):
            for condition, copy in far_copies(own_front, slot, t):
                drain(condition, copy)


def body(
    upper_a, upper_b, right_side, vectors_a, inverse_a, values_a, vectors_b, inverse_b, values_b
):
    tall = (N_SLOT, 2 * BLOCK, HALF)
    square = (N_SLOT, BLOCK, BLOCK)
    anywhere = pl.BlockSpec(memory_space=pl.ANY)
    inside = pl.BlockSpec(memory_space=pltpu.VMEM)
    dma = pltpu.SemaphoreType.DMA
    solved = pl.pallas_call(
        kernel,
        out_shape=pltpu.VMEM(tall, jnp.float32),
        in_specs=[anywhere] * 5 + [inside] + [anywhere] * 2 + [inside],
        out_specs=inside,
        scratch_shapes=[
            pltpu.VMEM((FRONTS, *tall), jnp.float32),
            pltpu.VMEM((FRONTS, *tall), jnp.float32),
            pltpu.VMEM(square, jnp.float32),
            pltpu.VMEM((FRONTS, *square), jnp.float32),
            pltpu.VMEM((FRONTS - 1, BLOCK, BLOCK), jnp.float32),
            *[pltpu.VMEM((BLOCK, BLOCK), jnp.float32)] * 5,
            dma((4, N_SLOT)),
            dma((4, N_SLOT)),
            dma((4, N_SLOT)),
            dma((4, N_SLOT)),
            dma((FRONTS // 2, N_SLOT, 2, 3)),
            dma((2, 3)),
            dma((FRONTS, N_SLOT, 2)),
            dma((2, 7)),
            dma((FRONTS, 2)),
            dma((2, 3)),
            dma((2, 3)),
            dma((7,)),
        ],
        compiler_params=pltpu.CompilerParams(
            collective_id=0, has_side_effects=True, vmem_limit_bytes=60 * 1024 * 1024
        ),
    )(
        upper_a.reshape(tall), upper_b.reshape(tall), right_side.reshape(tall),
        vectors_a.reshape(square), inverse_a.reshape(square), values_a.reshape(2 * N_SLOT, HALF),
        vectors_b.reshape(BLOCK, BLOCK), inverse_b.reshape(BLOCK, BLOCK), values_b.reshape(2, HALF),
    )
    return solved.reshape(right_side.shape)


def solution(mesh):
    finer = Mesh(mesh.devices.reshape(2, 4, 4, 4, 2), ROW + COL)
    whole = P(None, ROW, None, COL, None)
    placed = (
        whole, whole, whole,
        P(None, ROW, None, None), P(None, ROW, None, None), P(None, ROW, None),
        P(COL, None, None), P(COL, None, None), P(COL, None),
    )
    return jax.shard_map(body, mesh=finer, in_specs=placed, out_specs=whole, check_vma=False)
```
